128 devices in a mesh: px: 8 (over z_hi, y), py: 16 (over x, z_lo, core).
Axes of the slice: x: 4, y: 4, z: 4 (z_hi: 2, z_lo: 2; z = z_hi * 2 + z_lo), core: 2. Of those that a mesh axis runs over, the one named last changes fastest.
Arguments:
- white_noise: float32 [2, 128, 512, 256], P(None, 'px', 'py'), may hold values from -6 to 6
- spectrum: float32 [128, 512, 256], P('px', 'py'), may hold values from 0.1 to 2, as said below
- group_table: int32 [3, 16], replicated, may hold values from 0 to 15, each once within a row
Outputs:
- modulus: float32 [2, 128, 512, 256], P(None, 'px', 'py')
- level_one: float32 [2, 64, 256, 128], P(None, 'px', 'py')
- level_two: float32 [2, 32, 128, 64], P(None, 'px', 'py')
- level_three: float32 [2, 16, 64, 32], P(None, 'px', 'py')
The draws below stay inside these ranges and needn't reach their ends.
Inputs may be any that keep to these rules, and one draw needn't show every extreme that they name: spectrum[j, m, k] equals spectrum[(128 - j) % 128, (512 - m) % 512, (256 - k) % 256]. `group_table`: each row is a permutation of 0 to 15.
All inputs are finite; a program needn't handle non-finite values.
Results may differ from the reference program's by a relative error of at most 0.000088.
Values sent between devices are 32-bit elements; how exact they have to be, the bound alone decides.
A program may use at most 192 MiB of HBM per device.

```python
import math
import jax
import jax.numpy as jnp

FIELDS = 2
LEVELS = 3
NZ = 256
NX = 128
NY = 512
N_PY = 16


def draw_spectrum(key, part):
    log_low = math.log(0.1)
    log_high = math.log(2.0)
    rough_part = jnp.exp(jax.random.uniform(key, (NX, NY, NZ), jnp.float32, log_low, log_high))
    mirror = jnp.roll(jnp.flip(rough_part, (0, 1, 2)), 1, (0, 1, 2))
    values = 0.5 * (rough_part + mirror)
    return values


def level_of(stream_key, extent, shards, low, top_value):
    def one(axis_at, blocks):
        draws = jax.random.uniform(jax.random.fold_in(jax.random.fold_in(stream_key, 6), axis_at), (blocks,), jnp.float32, low / len(shards), top_value / len(shards))
        return jnp.repeat(jnp.exp(draws), extent[axis_at] // blocks).reshape((-1,) + (1,) * (len(extent) - axis_at - 1))

    level = one(*shards[0])
    for cut in shards[1:]:
        level = level * one(*cut)
    return level


def normal_values(own_key, shape, deviation, most, split=(), dtype=jnp.bfloat16):
    array = jax.random.normal(own_key, shape, jnp.float32) * deviation
    if len(split) > 0:
        array = level_of(own_key, shape, split, -0.22, 0.18) * array
    return jnp.clip(array, min=-most, max=most).astype(dtype)


def setup_inputs(seed: int = 0) -> dict:
    arg_keys = jax.random.split(jax.random.key(seed), 4)
    white_noise = normal_values(arg_keys[0], (FIELDS, NX, NY, NZ), 1.0, 6.0, ((1, 8), (2, 16)), jnp.float32)
    spectrum = draw_spectrum(jax.random.fold_in(arg_keys[3], 71), 0)
    group_table = jax.vmap(lambda own: jax.random.permutation(own, N_PY))(jax.random.split(arg_keys[2], LEVELS)).reshape((LEVELS, N_PY)).astype(jnp.int32)
    return dict(white_noise=white_noise, spectrum=spectrum, group_table=group_table)


def coarsen(values):
    members, size_x, size_y, size_z = values.shape
    blocks = values.reshape(members, size_x // 2, 2, size_y // 2, 2, size_z // 2, 2)
    return blocks.mean(axis=(2, 4, 6))


def route_blocks(coarse, group_order):
    members, size_x, size_y, size_z = coarse.shape
    blocks = coarse.reshape(members, size_x, N_PY, size_y // N_PY, size_z)
    picked = jnp.take(blocks, group_order, axis=2)
    return picked.reshape(members, size_x, size_y, size_z)


def reference(white_noise, spectrum, group_table):
    spectra = jnp.fft.fftn(white_noise, axes=(1, 2, 3))
    scaled = spectra * spectrum[None]
    fields_real = jnp.real(jnp.fft.ifftn(scaled, axes=(1, 2, 3)))
    modulus = jnp.exp(0.5 * fields_real)
    coarse_one = coarsen(modulus)
    coarse_two = coarsen(coarse_one)
    coarse_three = coarsen(coarse_two)
    level_one = route_blocks(coarse_one, group_table[0])
    level_two = route_blocks(coarse_two, group_table[1])
    level_three = route_blocks(coarse_three, group_table[2])
    return modulus, level_one, level_two, level_three
```

```python
import numpy as np

import jax
import jax.numpy as jnp
from jax import lax
from jax.experimental import pallas as pl
from jax.experimental.pallas import tpu as pltpu
from jax.sharding import PartitionSpec as P

MESH = pl.DeviceIdType.MESH
F32, BF16 = jnp.float32, jnp.bfloat16
PX, PY = 8, 16
DEV = PX * PY
LX, LY, LZ = 128, 512, 256
CX, CY = LX // PX, LY // PY
L = 128
QUAD = 4
HEIGHT = 24


def split(values):
    values = np.asarray(values, np.float32)
    high = values.astype(jnp.bfloat16)
    low = (values - high.astype(np.float32)).astype(jnp.bfloat16)
    return np.stack([high, low], 0)


def tables():
    k = np.arange(L)
    z = np.arange(LZ)
    angle = 2.0 * np.pi / LZ * (k[:, None] * z[None, :] % LZ)
    nyquist = np.where(z % 2 == 0, 1.0, -1.0)
    ahead = np.stack([np.cos(angle), -np.sin(angle)], 0)
    back = 2.0 * ahead
    ahead[1, 0] = nyquist
    back[0, 0] = 1.0
    back[1, 0] = nyquist
    z_ahead = split(ahead.reshape(LZ, LZ))
    z_back = split(back.reshape(LZ, LZ) / (LX * LY * LZ))
    first, second = k // 16, k % 16
    turn = first[:, None] * first[None, :] / 8.0 + second[:, None] * second[None, :] / 16.0
    cos, sin = np.cos(2 * np.pi * turn), -np.sin(2 * np.pi * turn)
    column = split(np.block([[cos, -sin], [sin, cos]]))
    row = split(np.block([[cos, sin], [-sin, cos]]))
    twiddle, small = [], []
    for t in range(QUAD):
        xl = (t // 2) * 8 + first
        yl = (t % 2) * 16 + second
        turn = first[:, None] * xl[None, :] / LX + second[:, None] * yl[None, :] / LY
        twiddle.append(np.stack([np.cos(2 * np.pi * turn), -np.sin(2 * np.pi * turn)], 0))
        turn = (t // 2) * first / 16.0 + (t % 2) * second / 32.0
        small.append(np.stack([np.cos(2 * np.pi * turn), -np.sin(2 * np.pi * turn)], 0))
    twiddle = np.concatenate(twiddle, 2).astype(np.float32)
    small = np.stack(small, 1).reshape(2 * QUAD, L).astype(np.float32)
    pool = np.zeros((LZ, LZ))
    pool[z, z // 2] = 1.0 / 8
    pool[z, 128 + z // 4] = 1.0 / 64
    pool[z, 192 + z // 8] = 1.0 / 512
    return [
        jnp.asarray(v)
        for v in (z_ahead, z_back, column, row, twiddle, small, pool.astype(jnp.bfloat16))
    ]


def parts(values):
    high = values.astype(BF16)
    return high, (values - high.astype(F32)).astype(BF16)


def product(left, right, dims):
    return lax.dot_general(left, right, (dims, ((), ())), preferred_element_type=F32)


def left_table(table, values, dims=((1,), (0,))):
    high, low = parts(values)
    first = product(table[0], high, dims) + product(table[0], low, dims)
    return first + product(table[1], high, dims)


def right_table(values, table, dims=((1,), (0,))):
    high, low = parts(values)
    first = product(high, table[0], dims) + product(low, table[0], dims)
    return first + product(high, table[1], dims)


def peer(index):
    return {"px": index // PY, "py": lax.rem(index, PY)}


def quarter(t):
    return slice((t // 2) * 8, (t // 2) * 8 + 8), slice((t % 2) * 16, (t % 2) * 16 + 16)


def tile(t):
    return slice(t * L, (t + 1) * L)


def butterfly(values):
    a, b, c, d = values
    p, q, r, s = a + b, a - b, c + d, c - d
    return [p + r, q + s, p - r, q - s]


def turned(real, imag, cos, sin):
    return real * cos - imag * sin, real * sin + imag * cos


def piece(index, height):
    return pl.ds(pl.multiple_of(index * height, height), height)


def kernel(
    group_ref, noise_ref, spec_ref, za_ref, zb_ref, col_ref, row_ref, tw_ref, small_ref, pool_ref,
    mod_ref, one_ref, two_ref, three_ref,
    s_send, s_recv, n_send, n_recv, u_table, v_table, ahead_send, ahead_recv, back_send, back_recv,
    half_y, c_send, c_recv, d_send, d_recv, local_sems, send_sems, recv_sems,
):
    me = lax.axis_index("px") * PY + lax.axis_index("py")
    my_py = lax.axis_index("py")
    barrier = pltpu.get_barrier_semaphore()

    @pl.loop(1, DEV)
    def _(away):
        other = lax.rem(me + away, DEV)
        pl.semaphore_signal(barrier, inc=1, device_id=peer(other), device_id_type=MESH)

    def spread(send, recv, height, slot):
        pltpu.make_async_copy(
            send.at[piece(me, height)], recv.at[piece(me, height)], local_sems.at[slot]
        ).start()

        @pl.loop(1, DEV)
        def _(away):
            other = lax.rem(me + away, DEV)
            pltpu.make_async_remote_copy(
                src_ref=send.at[piece(other, height)],
                dst_ref=recv.at[piece(me, height)],
                send_sem=send_sems.at[slot],
                recv_sem=recv_sems.at[slot],
                device_id=peer(other),
                device_id_type=MESH,
            ).start()

    def landed(send, recv, height, slot):
        pltpu.make_async_copy(
            send.at[piece(me, height)], recv.at[piece(me, height)], local_sems.at[slot]
        ).wait()
        rest = pl.ds(0, (DEV - 1) * height)
        whole = pltpu.make_async_remote_copy(
            src_ref=send.at[rest],
            dst_ref=recv.at[rest],
            send_sem=send_sems.at[slot],
            recv_sem=recv_sems.at[slot],
            device_id=peer(lax.rem(me + 1, DEV)),
            device_id_type=MESH,
        )
        whole.wait()

    for t in range(QUAD):
        xs, ys = quarter(t)
        block = spec_ref[xs, ys, :].reshape(L, LZ)
        s_send[pl.ds(t, L, stride=QUAD), :] = block[:, :L].T
        n_send[pl.ds(t, 1), :] = block[:, L:].T[:1]

    za = (za_ref[0], za_ref[1])

    def z_ahead(f):
        rows = [noise_ref[(f,) + quarter(t)].reshape(L, LZ) for t in range(QUAD)]
        return left_table(za, jnp.concatenate(rows, 0), ((1,), (1,)))

    values = [z_ahead(0), z_ahead(1)]
    at_zero = lax.broadcasted_iota(jnp.int32, (L, QUAD * L), 0) == 0
    real_one = jnp.where(at_zero, values[0][L:], values[1][:L])
    imag_zero = jnp.where(at_zero, values[1][:L], values[0][L:])
    members = ((values[0][:L], imag_zero), (real_one, values[1][L:]))
    for f in range(2):
        for c in range(2):
            for t in range(QUAD):
                ahead_send[f, pl.ds(c * QUAD + t, L, stride=8), :] = members[f][c][:, tile(t)]

    pl.semaphore_wait(barrier, DEV - 1)
    spread(s_send, s_recv, QUAD, 0)

    def last_copy(source):
        return pltpu.make_async_remote_copy(
            src_ref=n_send,
            dst_ref=n_recv.at[source],
            send_sem=send_sems.at[5],
            recv_sem=recv_sems.at[5],
            device_id={"px": 0, "py": 0},
            device_id_type=MESH,
        )

    pl.when(me != 0)(lambda: last_copy(me).start())
    spread(ahead_send.at[0], ahead_recv.at[0], 8, 1)
    spread(ahead_send.at[1], ahead_recv.at[1], 8, 2)

    landed(s_send, s_recv, QUAD, 0)
    for t in range(QUAD):
        u_table[t] = s_recv[pl.ds(t, L, stride=QUAD), :].T

    @pl.when(me != 0)
    def _():
        v_table[...] = u_table[...]
        last_copy(me).wait_send()

    @pl.when(me == 0)
    def _():
        n_recv[0] = n_send[...]
        whole = pltpu.make_async_remote_copy(
            src_ref=n_recv.at[pl.ds(1, DEV - 1)],
            dst_ref=n_recv.at[pl.ds(1, DEV - 1)],
            send_sem=send_sems.at[5],
            recv_sem=recv_sems.at[5],
            device_id={"px": 0, "py": 1},
            device_id_type=MESH,
        )
        whole.wait_recv()
        for t in range(QUAD):
            v_table[t] = n_recv[:, t, :].T

    column = (col_ref[0], col_ref[1])
    row = (row_ref[0], row_ref[1])
    for f in range(2):
        landed(ahead_send.at[f], ahead_recv.at[f], 8, 1 + f)
        plane = [
            jnp.concatenate(
                [ahead_recv[f, pl.ds(c * QUAD + t, L, stride=8), :] for t in range(QUAD)], 1
            )
            for c in range(2)
        ]
        mixed = left_table(column, jnp.concatenate(plane, 0))
        real, imag = turned(mixed[:L], mixed[L:], tw_ref[0], tw_ref[1])
        reals = butterfly([real[:, tile(t)] for t in range(QUAD)])
        imags = butterfly([imag[:, tile(t)] for t in range(QUAD)])
        rows = []
        for t in range(QUAD):
            cos, sin = small_ref[pl.ds(t, 1), :], small_ref[pl.ds(QUAD + t, 1), :]
            pair = turned(reals[t], imags[t], cos, sin) if t else (reals[t], imags[t])
            rows.append(jnp.concatenate(pair, 1))
        freq = right_table(jnp.concatenate(rows, 0), row)
        table = u_table if f == 0 else v_table
        scale = jnp.concatenate([table[t] for t in range(QUAD)], 0)
        freq = freq * jnp.concatenate([scale, scale], 1)
        mixed = right_table(freq, column)
        reals, imags = [], []
        for t in range(QUAD):
            part = mixed[tile(t)]
            pair = (part[:, :L], part[:, L:])
            if t:
                cos, sin = small_ref[pl.ds(t, 1), :], small_ref[pl.ds(QUAD + t, 1), :]
                pair = turned(*pair, cos, -sin)
            reals.append(pair[0])
            imags.append(pair[1])
        real = jnp.concatenate(butterfly(reals), 1)
        imag = jnp.concatenate(butterfly(imags), 1)
        real, imag = turned(real, imag, tw_ref[0], -tw_ref[1])
        plane = left_table(row, jnp.concatenate([real, imag], 0))
        for c in range(2):
            for t in range(QUAD):
                back_send[f, pl.ds(c * QUAD + t, L, stride=8), :] = plane[tile(c), tile(t)]
        spread(back_send.at[f], back_recv.at[f], 8, 3 + f)

    for f in range(2):
        landed(back_send.at[f], back_recv.at[f], 8, 3 + f)

    def slot(f, c):
        rows = [back_recv[f, pl.ds(c * QUAD + t, L, stride=8), :] for t in range(QUAD)]
        return jnp.concatenate(rows, 1)

    middle = (slot(0, 1), slot(1, 0))
    imag_zero = jnp.where(at_zero, middle[1], middle[0])
    real_one = jnp.where(at_zero, middle[0], middle[1])
    members = ((slot(0, 0), imag_zero), (real_one, slot(1, 1)))
    zb = (zb_ref[0], zb_ref[1])

    def fold(start, rows):
        for h in range(2):
            half_y[h, pl.ds(start, rows.shape[0]), :] = rows[:, tile(h)]

    for f in range(2):
        cells = right_table(jnp.concatenate(members[f], 0), zb, ((0,), (0,)))
        cells = jnp.exp(0.5 * cells)
        for t in range(QUAD):
            xs, ys = quarter(t)
            block = cells[tile(t)].reshape(8, 16, LZ)
            mod_ref[f, xs, ys, :] = block
            half_x = block.reshape(4, 2, 16, LZ)
            half_x = half_x[:, 0] + half_x[:, 1]
            for x in range(4):
                fold(((f * 2 + t // 2) * 4 + x) * CY + (t % 2) * 16, half_x[x])

    def pair_rows(count):
        rows = [
            half_y[h, pl.ds(0, count, stride=2), :] + half_y[h, pl.ds(1, count, stride=2), :]
            for h in range(2)
        ]
        return jnp.concatenate(rows, 1)

    def z_pool(values, lanes):
        high, low = parts(values)
        pool = pool_ref[:, lanes]
        return product(high, pool, ((1,), (0,))) + product(low, pool, ((1,), (0,)))

    rows_one = pair_rows(2 * 8 * 16)
    one = z_pool(rows_one, slice(0, 128))
    pairs = rows_one.reshape(2 * 4, 2, 16, LZ)
    fold(0, (pairs[:, 0] + pairs[:, 1]).reshape(2 * 4 * 16, LZ))
    rows_two = pair_rows(2 * 4 * 8)
    pairs = rows_two.reshape(2 * 2, 2, 8, LZ)
    fold(0, (pairs[:, 0] + pairs[:, 1]).reshape(2 * 2 * 8, LZ))
    rows_three = pair_rows(2 * 2 * 4)
    rest = z_pool(jnp.concatenate([rows_two, rows_three], 0), slice(128, 256))
    for i in range(PY):
        c_send[i, pl.ds(0, 16), :] = one[i * 16 : i * 16 + 16]
        c_send[i, pl.ds(16, 4), :] = rest[i * 4 : i * 4 + 4]
        c_send[i, pl.ds(20, 1), :] = rest[64 + i : 65 + i]
        c_send[i, pl.ds(21, 3), :] = jnp.zeros((3, L), F32)

    def across(send, recv, slot):
        copies = [pltpu.make_async_copy(send.at[my_py], recv.at[my_py], local_sems.at[slot])]
        for away in range(1, PY):
            other = lax.rem(my_py + away, PY)
            copies.append(
                pltpu.make_async_remote_copy(
                    src_ref=send.at[other],
                    dst_ref=recv.at[my_py],
                    send_sem=send_sems.at[slot + away],
                    recv_sem=recv_sems.at[slot + away],
                    device_id={"py": other},
                    device_id_type=MESH,
                )
            )
        for copy in copies:
            copy.start()
        for copy in copies:
            copy.wait()

    across(c_send, c_recv, 6)
    for g in range(PY):
        for level, rows in enumerate((pl.ds(0, 16), pl.ds(16, 4), pl.ds(20, 1))):
            d_send[g, rows, :] = c_recv[group_ref[level, g], rows, :]
        d_send[g, pl.ds(21, 3), :] = jnp.zeros((3, L), F32)
    across(d_send, d_recv, 6 + PY)
    for f in range(2):
        for x in range(8):
            one_ref[f, x] = d_recv[f * 8 + x, pl.ds(0, 16), :]
        for x in range(4):
            for h in range(2):
                i = (f * 4 + x) * 2 + h
                two_ref[f, x, pl.ds(h * 4, 4), :] = d_recv[i, pl.ds(16, 4), :][:, :64]
        for x in range(2):
            for y in range(4):
                three_ref[f, x, pl.ds(y, 1), :] = d_recv[(f * 2 + x) * 4 + y, pl.ds(20, 1), :][:, 64:96]


def on_device(white_noise, spectrum, group_table):
    shapes = [
        white_noise.shape,
        (2, CX // 2, CY // 2, LZ // 2),
        (2, CX // 4, CY // 4, LZ // 4),
        (2, CX // 8, CY // 8, LZ // 8),
    ]
    vmem = pl.BlockSpec(memory_space=pltpu.VMEM)
    wide = pltpu.VMEM((2, DEV * 8, L), F32)
    thin = pltpu.VMEM((DEV * QUAD, L), F32)
    coarse = pltpu.VMEM((PY, HEIGHT, L), F32)
    slots = 6 + 2 * PY
    return pl.pallas_call(
        kernel,
        out_shape=[jax.ShapeDtypeStruct(shape, F32) for shape in shapes],
        in_specs=[pl.BlockSpec(memory_space=pltpu.SMEM)] + [vmem] * 9,
        out_specs=[vmem] * 4,
        scratch_shapes=[
            thin, thin, pltpu.VMEM((QUAD, L), F32), pltpu.VMEM((DEV, QUAD, L), F32),
            pltpu.VMEM((QUAD, L, L), F32), pltpu.VMEM((QUAD, L, L), F32),
            wide, wide, wide, wide,
            pltpu.VMEM((2, 2 * 8 * CY, L), F32), coarse, coarse, coarse, coarse,
            pltpu.SemaphoreType.DMA((slots,)), pltpu.SemaphoreType.DMA((slots,)),
            pltpu.SemaphoreType.DMA((slots,)),
        ],
        compiler_params=pltpu.CompilerParams(
            collective_id=0, has_side_effects=True, vmem_limit_bytes=48 * 1024 * 1024
        ),
    )(group_table, white_noise, spectrum, *tables())


def solution(mesh):
    in_specs = (P(None, "px", "py", None), P("px", "py", None), P())
    out_specs = (P(None, "px", "py", None),) * 4
    return jax.shard_map(
        on_device, mesh=mesh, in_specs=in_specs, out_specs=out_specs, check_vma=False
    )
```

```python
import numpy as np

import jax
import jax.numpy as jnp
from jax import lax
from jax.experimental import pallas as pl
from jax.experimental.pallas import tpu as pltpu
from jax.sharding import PartitionSpec as P

MESH = pl.DeviceIdType.MESH
F32, BF16 = jnp.float32, jnp.bfloat16
PX, PY = 8, 16
DEV = PX * PY
LX, LY, LZ = 128, 512, 256
CX, CY = LX // PX, LY // PY
L = 128
QUAD = 4
HEIGHT = 24


def split(values):
    values = np.asarray(values, np.float32)
    high = values.astype(jnp.bfloat16)
    low = (values - high.astype(np.float32)).astype(jnp.bfloat16)
    return np.stack([high, low], 0)


def tables():
    k = np.arange(L)
    z = np.arange(LZ)
    angle = 2.0 * np.pi / LZ * (k[:, None] * z[None, :] % LZ)
    nyquist = np.where(z % 2 == 0, 1.0, -1.0)
    ahead = np.stack([np.cos(angle), -np.sin(angle)], 0)
    back = 2.0 * ahead
    ahead[1, 0] = nyquist
    back[0, 0] = 1.0
    back[1, 0] = nyquist
    z_ahead = split(ahead.reshape(LZ, LZ))
    z_back = split(back.reshape(LZ, LZ) / (LX * LY * LZ))
    first, second = k // 16, k % 16
    turn = first[:, None] * first[None, :] / 8.0 + second[:, None] * second[None, :] / 16.0
    cos, sin = np.cos(2 * np.pi * turn), -np.sin(2 * np.pi * turn)
    column = split(np.block([[cos, -sin], [sin, cos]]))
    row = split(np.block([[cos, sin], [-sin, cos]]))
    twiddle, small = [], []
    for t in range(QUAD):
        xl = (t // 2) * 8 + first
        yl = (t % 2) * 16 + second
        turn = first[:, None] * xl[None, :] / LX + second[:, None] * yl[None, :] / LY
        twiddle.append(np.stack([np.cos(2 * np.pi * turn), -np.sin(2 * np.pi * turn)], 0))
        turn = (t // 2) * first / 16.0 + (t % 2) * second / 32.0
        small.append(np.stack([np.cos(2 * np.pi * turn), -np.sin(2 * np.pi * turn)], 0))
    twiddle = np.concatenate(twiddle, 2).astype(np.float32)
    small = np.stack(small, 1).reshape(2 * QUAD, L).astype(np.float32)
    pool = np.zeros((LZ, LZ))
    pool[z, z // 2] = 1.0 / 8
    pool[z, 128 + z // 4] = 1.0 / 64
    pool[z, 192 + z // 8] = 1.0 / 512
    return [
        jnp.asarray(v)
        for v in (z_ahead, z_back, column, row, twiddle, small, pool.astype(jnp.bfloat16))
    ]


def parts(values):
    high = values.astype(BF16)
    return high, (values - high.astype(F32)).astype(BF16)


def product(left, right, dims):
    return lax.dot_general(left, right, (dims, ((), ())), preferred_element_type=F32)


def left_table(table, values, dims=((1,), (0,))):
    high, low = parts(values)
    first = product(table[0], high, dims) + product(table[0], low, dims)
    return first + product(table[1], high, dims)


def right_table(values, table, dims=((1,), (0,))):
    high, low = parts(values)
    first = product(high, table[0], dims) + product(low, table[0], dims)
    return first + product(high, table[1], dims)


def place():
    px, py = lax.axis_index("px"), lax.axis_index("py")
    return (px >> 2) * 2 + ((py >> 1) & 1), px & 3, py >> 2, py & 1


def shifted(here, dz, dy, dx, dc):
    z, y, x = ((here[i] + d) & 3 for i, d in enumerate((dz, dy, dx)))
    px = (z >> 1) * 4 + y
    py = x * 4 + (z & 1) * 2 + (here[3] ^ dc)
    return px * PY + py, {"px": px, "py": py}


def quarter(t):
    return slice((t // 2) * 8, (t // 2) * 8 + 8), slice((t % 2) * 16, (t % 2) * 16 + 16)


def tile(t):
    return slice(t * L, (t + 1) * L)


def butterfly(values):
    a, b, c, d = values
    p, q, r, s = a + b, a - b, c + d, c - d
    return [p + r, q + s, p - r, q - s]


def turned(real, imag, cos, sin):
    return real * cos - imag * sin, real * sin + imag * cos


def piece(index, height):
    return pl.ds(pl.multiple_of(index * height, height), height)


def kernel(
    group_in, noise_in, spec_in, za_in, zb_in, col_in, row_in, tw_in, small_in, pool_in,
    mod_ref, one_ref, two_ref, three_ref,
    group_ref, noise_ref, spec_ref, za_ref, zb_ref, col_ref, row_ref, tw_ref, small_ref, pool_ref,
    s_send, s_recv, n_send, n_recv, u_table, v_table, ahead_send, ahead_recv, back_send, back_recv,
    half_y, c_send, c_recv, d_send, d_recv, all_sem, fetch_sems, local_sems, send_sems, recv_sems,
):
    here = place()
    my_px, my_py = lax.axis_index("px"), lax.axis_index("py")
    me = my_px * PY + my_py
    barrier = pltpu.get_barrier_semaphore()

    for away in range(1, PY):
        other = {"py": (my_py + away) & (PY - 1)}
        pl.semaphore_signal(barrier, inc=1, device_id=other, device_id_type=MESH)
    lines = [{"px": (my_px + away) & (PX - 1)} for away in range(1, PX)]
    for other in lines:
        pl.semaphore_signal(barrier, inc=1, device_id=other, device_id_type=MESH)
    pairs = (
        (spec_in, spec_ref), (noise_in, noise_ref), (za_in, za_ref), (col_in, col_ref),
        (row_in, row_ref), (tw_in, tw_ref), (small_in, small_ref), (zb_in, zb_ref),
        (pool_in, pool_ref), (group_in, group_ref),
    )
    fetches = [
        pltpu.make_async_copy(source, target, fetch_sems.at[index])
        for index, (source, target) in enumerate(pairs)
    ]
    for fetch in fetches:
        fetch.start()

    def spread(send, recv, height, slot):
        pltpu.make_async_copy(
            send.at[piece(me, height)], recv.at[piece(me, height)], local_sems.at[slot]
        ).start()

        def send_to(shift):
            other, device = shifted(here, *shift)
            pltpu.make_async_remote_copy(
                src_ref=send.at[piece(other, height)],
                dst_ref=recv.at[piece(me, height)],
                send_sem=send_sems.at[slot],
                recv_sem=recv_sems.at[slot],
                device_id=device,
                device_id_type=MESH,
            ).start()

        @pl.loop(0, 16)
        def _(step):
            dx, dy = step & 3, step >> 2
            pl.when(step != 0)(lambda: send_to((0, dy, dx, 0)))
            for n in range(1, 8):
                dz, dc = n >> 1, n & 1
                send_to((dz, dy + n, dx + dz, dc))

    def landed(send, recv, height, slot):
        pltpu.make_async_copy(
            send.at[piece(me, height)], recv.at[piece(me, height)], local_sems.at[slot]
        ).wait()
        rest = pl.ds(0, (DEV - 1) * height)
        whole = pltpu.make_async_remote_copy(
            src_ref=send.at[rest],
            dst_ref=recv.at[rest],
            send_sem=send_sems.at[slot],
            recv_sem=recv_sems.at[slot],
            device_id=shifted(here, 0, 0, 0, 1)[1],
            device_id_type=MESH,
        )
        whole.wait()

    fetches[0].wait()
    for t in range(QUAD):
        xs, ys = quarter(t)
        block = spec_ref[xs, ys, :].reshape(L, LZ)
        s_send[pl.ds(t, L, stride=QUAD), :] = block[:, :L].T
        n_send[pl.ds(t, 1), :] = block[:, L:].T[:1]

    pl.semaphore_wait(barrier, PX + PY - 2)
    for other in lines:
        pl.semaphore_signal(all_sem, inc=1, device_id=other, device_id_type=MESH)

    fetches[1].wait()
    fetches[2].wait()
    za = (za_ref[0], za_ref[1])

    def z_ahead(f):
        rows = [noise_ref[(f,) + quarter(t)].reshape(L, LZ) for t in range(QUAD)]
        return left_table(za, jnp.concatenate(rows, 0), ((1,), (1,)))

    values = [z_ahead(0), z_ahead(1)]
    at_zero = lax.broadcasted_iota(jnp.int32, (L, QUAD * L), 0) == 0
    real_one = jnp.where(at_zero, values[0][L:], values[1][:L])
    imag_zero = jnp.where(at_zero, values[1][:L], values[0][L:])
    members = ((values[0][:L], imag_zero), (real_one, values[1][L:]))
    for f in range(2):
        for c in range(2):
            for t in range(QUAD):
                ahead_send[f, pl.ds(c * QUAD + t, L, stride=8), :] = members[f][c][:, tile(t)]

    pl.semaphore_wait(all_sem, PX - 1)
    spread(s_send, s_recv, QUAD, 0)

    def last_copy(source):
        return pltpu.make_async_remote_copy(
            src_ref=n_send,
            dst_ref=n_recv.at[source],
            send_sem=send_sems.at[5],
            recv_sem=recv_sems.at[5],
            device_id={"px": 0, "py": 0},
            device_id_type=MESH,
        )

    pl.when(me != 0)(lambda: last_copy(me).start())
    spread(ahead_send.at[0], ahead_recv.at[0], 8, 1)
    spread(ahead_send.at[1], ahead_recv.at[1], 8, 2)

    landed(s_send, s_recv, QUAD, 0)
    for t in range(QUAD):
        u_table[t] = s_recv[pl.ds(t, L, stride=QUAD), :].T

    @pl.when(me != 0)
    def _():
        v_table[...] = u_table[...]
        last_copy(me).wait_send()

    @pl.when(me == 0)
    def _():
        n_recv[0] = n_send[...]
        whole = pltpu.make_async_remote_copy(
            src_ref=n_recv.at[pl.ds(1, DEV - 1)],
            dst_ref=n_recv.at[pl.ds(1, DEV - 1)],
            send_sem=send_sems.at[5],
            recv_sem=recv_sems.at[5],
            device_id={"px": 0, "py": 1},
            device_id_type=MESH,
        )
        whole.wait_recv()
        for t in range(QUAD):
            v_table[t] = n_recv[:, t, :].T

    for index in range(3, 7):
        fetches[index].wait()
    column = (col_ref[0], col_ref[1])
    row = (row_ref[0], row_ref[1])
    for f in range(2):
        landed(ahead_send.at[f], ahead_recv.at[f], 8, 1 + f)
        plane = [
            jnp.concatenate(
                [ahead_recv[f, pl.ds(c * QUAD + t, L, stride=8), :] for t in range(QUAD)], 1
            )
            for c in range(2)
        ]
        mixed = left_table(column, jnp.concatenate(plane, 0))
        real, imag = turned(mixed[:L], mixed[L:], tw_ref[0], tw_ref[1])
        reals = butterfly([real[:, tile(t)] for t in range(QUAD)])
        imags = butterfly([imag[:, tile(t)] for t in range(QUAD)])
        rows = []
        for t in range(QUAD):
            cos, sin = small_ref[pl.ds(t, 1), :], small_ref[pl.ds(QUAD + t, 1), :]
            pair = turned(reals[t], imags[t], cos, sin) if t else (reals[t], imags[t])
            rows.append(jnp.concatenate(pair, 1))
        freq = right_table(jnp.concatenate(rows, 0), row)
        table = u_table if f == 0 else v_table
        scale = jnp.concatenate([table[t] for t in range(QUAD)], 0)
        freq = freq * jnp.concatenate([scale, scale], 1)
        mixed = right_table(freq, column)
        reals, imags = [], []
        for t in range(QUAD):
            part = mixed[tile(t)]
            pair = (part[:, :L], part[:, L:])
            if t:
                cos, sin = small_ref[pl.ds(t, 1), :], small_ref[pl.ds(QUAD + t, 1), :]
                pair = turned(*pair, cos, -sin)
            reals.append(pair[0])
            imags.append(pair[1])
        real = jnp.concatenate(butterfly(reals), 1)
        imag = jnp.concatenate(butterfly(imags), 1)
        real, imag = turned(real, imag, tw_ref[0], -tw_ref[1])
        plane = left_table(row, jnp.concatenate([real, imag], 0))
        for c in range(2):
            for t in range(QUAD):
                back_send[f, pl.ds(c * QUAD + t, L, stride=8), :] = plane[tile(c), tile(t)]
        spread(back_send.at[f], back_recv.at[f], 8, 3 + f)

    for f in range(2):
        landed(back_send.at[f], back_recv.at[f], 8, 3 + f)

    def slot(f, c):
        rows = [back_recv[f, pl.ds(c * QUAD + t, L, stride=8), :] for t in range(QUAD)]
        return jnp.concatenate(rows, 1)

    for index in range(7, 10):
        fetches[index].wait()
    middle = (slot(0, 1), slot(1, 0))
    imag_zero = jnp.where(at_zero, middle[1], middle[0])
    real_one = jnp.where(at_zero, middle[0], middle[1])
    members = ((slot(0, 0), imag_zero), (real_one, slot(1, 1)))
    zb = (zb_ref[0], zb_ref[1])

    def fold(start, rows):
        for h in range(2):
            half_y[h, pl.ds(start, rows.shape[0]), :] = rows[:, tile(h)]

    for f in range(2):
        cells = right_table(jnp.concatenate(members[f], 0), zb, ((0,), (0,)))
        cells = jnp.exp(0.5 * cells)
        for t in range(QUAD):
            xs, ys = quarter(t)
            block = cells[tile(t)].reshape(8, 16, LZ)
            mod_ref[f, xs, ys, :] = block
            half_x = block.reshape(4, 2, 16, LZ)
            half_x = half_x[:, 0] + half_x[:, 1]
            for x in range(4):
                fold(((f * 2 + t // 2) * 4 + x) * CY + (t % 2) * 16, half_x[x])

    def pair_rows(count):
        rows = [
            half_y[h, pl.ds(0, count, stride=2), :] + half_y[h, pl.ds(1, count, stride=2), :]
            for h in range(2)
        ]
        return jnp.concatenate(rows, 1)

    def z_pool(values, lanes):
        high, low = parts(values)
        pool = pool_ref[:, lanes]
        return product(high, pool, ((1,), (0,))) + product(low, pool, ((1,), (0,)))

    rows_one = pair_rows(2 * 8 * 16)
    one = z_pool(rows_one, slice(0, 128))
    pairs = rows_one.reshape(2 * 4, 2, 16, LZ)
    fold(0, (pairs[:, 0] + pairs[:, 1]).reshape(2 * 4 * 16, LZ))
    rows_two = pair_rows(2 * 4 * 8)
    pairs = rows_two.reshape(2 * 2, 2, 8, LZ)
    fold(0, (pairs[:, 0] + pairs[:, 1]).reshape(2 * 2 * 8, LZ))
    rows_three = pair_rows(2 * 2 * 4)
    rest = z_pool(jnp.concatenate([rows_two, rows_three], 0), slice(128, 256))
    for i in range(PY):
        c_send[i, pl.ds(0, 16), :] = one[i * 16 : i * 16 + 16]
        c_send[i, pl.ds(16, 4), :] = rest[i * 4 : i * 4 + 4]
        c_send[i, pl.ds(20, 1), :] = rest[64 + i : 65 + i]
        c_send[i, pl.ds(21, 3), :] = jnp.zeros((3, L), F32)

    def across(send, recv, slot):
        copies = [pltpu.make_async_copy(send.at[my_py], recv.at[my_py], local_sems.at[slot])]
        for away in range(1, PY):
            other = lax.rem(my_py + away, PY)
            copies.append(
                pltpu.make_async_remote_copy(
                    src_ref=send.at[other],
                    dst_ref=recv.at[my_py],
                    send_sem=send_sems.at[slot + away],
                    recv_sem=recv_sems.at[slot + away],
                    device_id={"py": other},
                    device_id_type=MESH,
                )
            )
        for copy in copies:
            copy.start()
        for copy in copies:
            copy.wait()

    across(c_send, c_recv, 6)
    for g in range(PY):
        for level, rows in enumerate((pl.ds(0, 16), pl.ds(16, 4), pl.ds(20, 1))):
            d_send[g, rows, :] = c_recv[group_ref[level, g], rows, :]
        d_send[g, pl.ds(21, 3), :] = jnp.zeros((3, L), F32)
    across(d_send, d_recv, 6 + PY)
    for f in range(2):
        for x in range(8):
            one_ref[f, x] = d_recv[f * 8 + x, pl.ds(0, 16), :]
        for x in range(4):
            for h in range(2):
                i = (f * 4 + x) * 2 + h
                two_ref[f, x, pl.ds(h * 4, 4), :] = d_recv[i, pl.ds(16, 4), :][:, :64]
        for x in range(2):
            for y in range(4):
                three_ref[f, x, pl.ds(y, 1), :] = d_recv[(f * 2 + x) * 4 + y, pl.ds(20, 1), :][:, 64:96]


def on_device(white_noise, spectrum, group_table):
    shapes = [
        white_noise.shape,
        (2, CX // 2, CY // 2, LZ // 2),
        (2, CX // 4, CY // 4, LZ // 4),
        (2, CX // 8, CY // 8, LZ // 8),
    ]
    vmem = pl.BlockSpec(memory_space=pltpu.VMEM)
    hbm = pl.BlockSpec(memory_space=pltpu.HBM)
    wide = pltpu.VMEM((2, DEV * 8, L), F32)
    thin = pltpu.VMEM((DEV * QUAD, L), F32)
    coarse = pltpu.VMEM((PY, HEIGHT, L), F32)
    slots = 6 + 2 * PY
    operands = [white_noise, spectrum] + tables()
    return pl.pallas_call(
        kernel,
        out_shape=[jax.ShapeDtypeStruct(shape, F32) for shape in shapes],
        in_specs=[hbm] * (len(operands) + 1),
        out_specs=[vmem] * 4,
        scratch_shapes=[pltpu.SMEM(group_table.shape, jnp.int32)]
        + [pltpu.VMEM(value.shape, value.dtype) for value in operands]
        + [
            thin, thin, pltpu.VMEM((QUAD, L), F32), pltpu.VMEM((DEV, QUAD, L), F32),
            pltpu.VMEM((QUAD, L, L), F32), pltpu.VMEM((QUAD, L, L), F32),
            wide, wide, wide, wide,
            pltpu.VMEM((2, 2 * 8 * CY, L), F32), coarse, coarse, coarse, coarse,
            pltpu.SemaphoreType.REGULAR, pltpu.SemaphoreType.DMA((len(operands) + 1,)), pltpu.SemaphoreType.DMA((slots,)), pltpu.SemaphoreType.DMA((slots,)),
            pltpu.SemaphoreType.DMA((slots,)),
        ],
        compiler_params=pltpu.CompilerParams(
            collective_id=0, has_side_effects=True, vmem_limit_bytes=67_043_328
        ),
    )(group_table, *operands)


def solution(mesh):
    in_specs = (P(None, "px", "py", None), P("px", "py", None), P())
    out_specs = (P(None, "px", "py", None),) * 4
    return jax.shard_map(
        on_device, mesh=mesh, in_specs=in_specs, out_specs=out_specs, check_vma=False
    )
```

```python
import numpy as np

import jax
import jax.numpy as jnp
from jax import lax
from jax.experimental import pallas as pl
from jax.experimental.pallas import tpu as pltpu
from jax.sharding import PartitionSpec as P

MESH = pl.DeviceIdType.MESH
F32, BF16 = jnp.float32, jnp.bfloat16
PX, PY = 8, 16
DEV = PX * PY
LX, LY, LZ = 128, 512, 256
CX, CY = LX // PX, LY // PY
L = 128
QUAD = 4


def split(values):
    values = np.asarray(values, np.float32)
    high = values.astype(jnp.bfloat16)
    low = (values - high.astype(np.float32)).astype(jnp.bfloat16)
    return np.stack([high, low], 0)


def tables():
    k = np.arange(L)
    z = np.arange(LZ)
    angle = 2.0 * np.pi / LZ * (k[:, None] * z[None, :] % LZ)
    nyquist = np.where(z % 2 == 0, 1.0, -1.0)
    ahead = np.stack([np.cos(angle), -np.sin(angle)], 0)
    back = 2.0 * ahead
    ahead[1, 0] = nyquist
    back[0, 0] = 1.0
    back[1, 0] = nyquist
    z_ahead = split(ahead.reshape(LZ, LZ))
    z_back = split(back.reshape(LZ, LZ) / (LX * LY * LZ))
    first, second = k // 16, k % 16
    turn = first[:, None] * first[None, :] / 8.0 + second[:, None] * second[None, :] / 16.0
    cos, sin = np.cos(2 * np.pi * turn), -np.sin(2 * np.pi * turn)
    column = split(np.block([[cos, -sin], [sin, cos]]))
    row = split(np.block([[cos, sin], [-sin, cos]]))
    twiddle, small = [], []
    for t in range(QUAD):
        xl = (t // 2) * 8 + first
        yl = (t % 2) * 16 + second
        turn = first[:, None] * xl[None, :] / LX + second[:, None] * yl[None, :] / LY
        twiddle.append(np.stack([np.cos(2 * np.pi * turn), -np.sin(2 * np.pi * turn)], 0))
        turn = (t // 2) * first / 16.0 + (t % 2) * second / 32.0
        small.append(np.stack([np.cos(2 * np.pi * turn), -np.sin(2 * np.pi * turn)], 0))
    twiddle = np.concatenate(twiddle, 2).astype(np.float32)
    small = np.stack(small, 1).reshape(2 * QUAD, L).astype(np.float32)
    pool = np.zeros((LZ, LZ))
    pool[z, z // 2] = 1.0 / 8
    pool[z, 128 + z // 4] = 1.0 / 64
    pool[z, 192 + z // 8] = 1.0 / 512
    return [
        jnp.asarray(v)
        for v in (z_ahead, z_back, column, row, twiddle, small, pool.astype(jnp.bfloat16))
    ]


def parts(values):
    high = values.astype(BF16)
    return high, (values - high.astype(F32)).astype(BF16)


def product(left, right, dims):
    return lax.dot_general(left, right, (dims, ((), ())), preferred_element_type=F32)


def left_table(table, values, dims=((1,), (0,))):
    high, low = parts(values)
    first = product(table[0], high, dims) + product(table[0], low, dims)
    return first + product(table[1], high, dims)


def right_table(values, table, dims=((1,), (0,))):
    high, low = parts(values)
    first = product(high, table[0], dims) + product(low, table[0], dims)
    return first + product(high, table[1], dims)


def hops(shift):
    return sum(min(d, 4 - d) for d in shift[:3])


SHIFTS = [(dz, dy, dx, dc) for dz in range(4) for dy in range(4) for dx in range(4) for dc in range(2)]
MIXED = [SHIFTS[(i * 37) % 128] for i in range(1, 128)]
SHIFTS = sorted(SHIFTS[1:], key=lambda shift: -hops(shift))

LINE = [(dx, low) for dx in range(4) for low in range(4)]
LINE = sorted(LINE[1:], key=lambda move: -min(move[0], 4 - move[0]) - (move[1] >> 1))


def place():
    px, py = lax.axis_index("px"), lax.axis_index("py")
    return (px >> 2) * 2 + ((py >> 1) & 1), px & 3, py >> 2, py & 1


def shifted(here, dz, dy, dx, dc):
    z, y, x = ((here[i] + d) & 3 for i, d in enumerate((dz, dy, dx)))
    px = (z >> 1) * 4 + y
    py = x * 4 + (z & 1) * 2 + (here[3] ^ dc)
    return px * PY + py, {"px": px, "py": py}


def quarter(t):
    return slice((t // 2) * 8, (t // 2) * 8 + 8), slice((t % 2) * 16, (t % 2) * 16 + 16)


def tile(t):
    return slice(t * L, (t + 1) * L)


def butterfly(values):
    a, b, c, d = values
    p, q, r, s = a + b, a - b, c + d, c - d
    return [p + r, q + s, p - r, q - s]


def turned(real, imag, cos, sin):
    return real * cos - imag * sin, real * sin + imag * cos


def piece(index, height):
    return pl.ds(pl.multiple_of(index * height, height), height)


def kernel(
    group_in, noise_in, spec_in, za_in, zb_in, col_in, row_in, tw_in, small_in, pool_in,
    mod_out, one_out, rest_out,
    group_ref, noise_ref, spec_ref, za_ref, zb_ref, col_ref, row_ref, tw_ref, small_ref, pool_ref,
    s_send, s_recv, n_send, n_line, n_recv, u_table, v_table, ahead_send, ahead_recv, back_send, back_recv,
    mod_ref, half_y, one_send, one_recv_0, one_recv_1, one_back, rest_send, rest_recv, rest_back,
    fetch_sems, local_sems, send_sems, recv_sems,
):
    here = place()
    my_px, my_py = lax.axis_index("px"), lax.axis_index("py")
    me = my_px * PY + my_py
    barrier = pltpu.get_barrier_semaphore()

    pairs = (
        (spec_in, spec_ref), (noise_in, noise_ref), (za_in, za_ref), (col_in, col_ref),
        (row_in, row_ref), (tw_in, tw_ref), (small_in, small_ref), (zb_in, zb_ref),
        (pool_in, pool_ref), (group_in, group_ref),
    )
    fetches = [
        pltpu.make_async_copy(source, target, fetch_sems.at[index])
        for index, (source, target) in enumerate(pairs)
    ]
    for fetch in fetches:
        fetch.start()

    for shift in SHIFTS:
        pl.semaphore_signal(barrier, inc=1, device_id=shifted(here, *shift)[1], device_id_type=MESH)

    def spread(send, recv, height, slot, order=MIXED):
        pltpu.make_async_copy(
            send.at[piece(me, height)], recv.at[piece(me, height)], local_sems.at[slot]
        ).start()

        def send_to(shift):
            other, device = shifted(here, *shift)
            pltpu.make_async_remote_copy(
                src_ref=send.at[piece(other, height)],
                dst_ref=recv.at[piece(me, height)],
                send_sem=send_sems.at[slot],
                recv_sem=recv_sems.at[slot],
                device_id=device,
                device_id_type=MESH,
            ).start()

        for shift in order:
            send_to(shift)

    def landed(send, recv, height, slot):
        pltpu.make_async_copy(
            send.at[piece(me, height)], recv.at[piece(me, height)], local_sems.at[slot]
        ).wait()
        rest = pl.ds(0, (DEV - 1) * height)
        whole = pltpu.make_async_remote_copy(
            src_ref=send.at[rest],
            dst_ref=recv.at[rest],
            send_sem=send_sems.at[slot],
            recv_sem=recv_sems.at[slot],
            device_id=shifted(here, 0, 0, 0, 1)[1],
            device_id_type=MESH,
        )
        whole.wait()

    fetches[0].wait()
    for t in range(QUAD):
        xs, ys = quarter(t)
        block = spec_ref[xs, ys, :].reshape(L, LZ)
        s_send[pl.ds(t, L, stride=QUAD), :] = block[:, :L].T
        n_send[pl.ds(t, 1), :] = block[:, L:].T[:1]

    fetches[1].wait()
    fetches[2].wait()
    za = (za_ref[0], za_ref[1])

    def z_ahead(f):
        rows = [noise_ref[(f,) + quarter(t)].reshape(L, LZ) for t in range(QUAD)]
        return left_table(za, jnp.concatenate(rows, 0), ((1,), (1,)))

    values = [z_ahead(0), z_ahead(1)]
    at_zero = lax.broadcasted_iota(jnp.int32, (L, QUAD * L), 0) == 0
    real_one = jnp.where(at_zero, values[0][L:], values[1][:L])
    imag_zero = jnp.where(at_zero, values[1][:L], values[0][L:])
    members = ((values[0][:L], imag_zero), (real_one, values[1][L:]))
    for f in range(2):
        for c in range(2):
            for t in range(QUAD):
                ahead_send[f, pl.ds(c * QUAD + t, L, stride=8), :] = members[f][c][:, tile(t)]

    pl.semaphore_wait(barrier, DEV - 1)
    line_copy = pltpu.make_async_remote_copy(
        src_ref=n_send,
        dst_ref=n_line.at[my_py],
        send_sem=send_sems.at[5],
        recv_sem=recv_sems.at[5],
        device_id={"py": 0},
        device_id_type=MESH,
    )
    plane_copies = [
        pltpu.make_async_remote_copy(
            src_ref=n_line.at[i],
            dst_ref=n_recv.at[my_px * PY + i],
            send_sem=send_sems.at[6],
            recv_sem=recv_sems.at[6],
            device_id={"px": 0},
            device_id_type=MESH,
        )
        for i in range(PY)
    ]

    def line_rest(device):
        rest = n_line.at[pl.ds(1, PY - 1)]
        return pltpu.make_async_remote_copy(
            src_ref=rest, dst_ref=rest, send_sem=send_sems.at[5], recv_sem=recv_sems.at[5],
            device_id=device, device_id_type=MESH,
        )

    def plane_rest(rest, device):
        return pltpu.make_async_remote_copy(
            src_ref=rest, dst_ref=rest, send_sem=send_sems.at[6], recv_sem=recv_sems.at[6],
            device_id=device, device_id_type=MESH,
        )

    pl.when(my_py != 0)(line_copy.start)
    spread(s_send, s_recv, QUAD, 0)

    spread(ahead_send.at[0], ahead_recv.at[0], 8, 1)

    @pl.when(my_py == 0)
    def _():
        n_line[0] = n_send[...]
        line_rest({"py": 1}).wait_recv()

        @pl.when(my_px != 0)
        def _():
            for copy in plane_copies:
                copy.start()

    spread(ahead_send.at[1], ahead_recv.at[1], 8, 2)

    landed(s_send, s_recv, QUAD, 0)
    for t in range(QUAD):
        u_table[t] = s_recv[pl.ds(t, L, stride=QUAD), :].T

    pl.when(my_py != 0)(line_copy.wait_send)
    for index in range(3, 7):
        fetches[index].wait()

    def last_table():
        @pl.when(me != 0)
        def _():
            v_table[...] = u_table[...]

        @pl.when((my_py == 0) & (my_px != 0))
        def _():
            plane_rest(n_line, {"px": 0}).wait_send()

        @pl.when(me == 0)
        def _():
            n_recv[pl.ds(0, PY)] = n_line[...]
            plane_rest(n_recv.at[pl.ds(PY, DEV - PY)], {"px": 1}).wait_recv()
            for t in range(QUAD):
                v_table[t] = n_recv[:, t, :].T

    column = (col_ref[0], col_ref[1])
    row = (row_ref[0], row_ref[1])
    for f in range(2):
        landed(ahead_send.at[f], ahead_recv.at[f], 8, 1 + f)
        if f == 1:
            last_table()
        plane = [
            jnp.concatenate(
                [ahead_recv[f, pl.ds(c * QUAD + t, L, stride=8), :] for t in range(QUAD)], 1
            )
            for c in range(2)
        ]
        mixed = left_table(column, jnp.concatenate(plane, 0))
        real, imag = turned(mixed[:L], mixed[L:], tw_ref[0], tw_ref[1])
        reals = butterfly([real[:, tile(t)] for t in range(QUAD)])
        imags = butterfly([imag[:, tile(t)] for t in range(QUAD)])
        rows = []
        for t in range(QUAD):
            cos, sin = small_ref[pl.ds(t, 1), :], small_ref[pl.ds(QUAD + t, 1), :]
            pair = turned(reals[t], imags[t], cos, sin) if t else (reals[t], imags[t])
            rows.append(jnp.concatenate(pair, 1))
        freq = right_table(jnp.concatenate(rows, 0), row)
        table = u_table if f == 0 else v_table
        scale = jnp.concatenate([table[t] for t in range(QUAD)], 0)
        freq = freq * jnp.concatenate([scale, scale], 1)
        mixed = right_table(freq, column)
        reals, imags = [], []
        for t in range(QUAD):
            part = mixed[tile(t)]
            pair = (part[:, :L], part[:, L:])
            if t:
                cos, sin = small_ref[pl.ds(t, 1), :], small_ref[pl.ds(QUAD + t, 1), :]
                pair = turned(*pair, cos, -sin)
            reals.append(pair[0])
            imags.append(pair[1])
        real = jnp.concatenate(butterfly(reals), 1)
        imag = jnp.concatenate(butterfly(imags), 1)
        real, imag = turned(real, imag, tw_ref[0], -tw_ref[1])
        plane = left_table(row, jnp.concatenate([real, imag], 0))
        for c in range(2):
            for t in range(QUAD):
                back_send[f, pl.ds(c * QUAD + t, L, stride=8), :] = plane[tile(c), tile(t)]
        if f == 0:
            pl.when(me != 0)(lambda: spread(back_send.at[0], back_recv.at[0], 8, 3, SHIFTS))
        else:

            @pl.when(me == 0)
            def _():
                for t in range(QUAD):
                    first, second = pl.ds(QUAD + t, L, stride=8), pl.ds(t, L, stride=8)
                    held = back_send[0, first, :], back_send[1, second, :]
                    back_send[0, first, :], back_send[1, second, :] = held[1], held[0]
                spread(back_send.at[0], back_recv.at[0], 8, 3, SHIFTS)

            spread(back_send.at[1], back_recv.at[1], 8, 4, SHIFTS)

    for index in range(7, 10):
        fetches[index].wait()
    zb = (zb_ref[0], zb_ref[1])

    def fold(start, rows):
        for h in range(2):
            half_y[h, pl.ds(start, rows.shape[0]), :] = rows[:, tile(h)]

    def pair_rows(start, count):
        rows = [
            half_y[h, pl.ds(start, count, stride=2), :] + half_y[h, pl.ds(start + 1, count, stride=2), :]
            for h in range(2)
        ]
        return jnp.concatenate(rows, 1)

    def z_pool(values, lanes):
        high, low = parts(values)
        pool = pool_ref[:, lanes]
        return product(high, pool, ((1,), (0,))) + product(low, pool, ((1,), (0,)))

    def across(send, recv, slot):
        copies = [pltpu.make_async_copy(send.at[my_py], recv.at[my_py], local_sems.at[slot])]
        for dx, low in LINE:
            other = (((my_py >> 2) + dx) & 3) * 4 + ((my_py & 3) ^ low)
            copies.append(
                pltpu.make_async_remote_copy(
                    src_ref=send.at[other],
                    dst_ref=recv.at[my_py],
                    send_sem=send_sems.at[slot + len(copies)],
                    recv_sem=recv_sems.at[slot + len(copies)],
                    device_id={"py": other},
                    device_id_type=MESH,
                )
            )
        for copy in copies:
            copy.start()
        return copies

    def coarse(f):
        tiles = [
            [back_recv[f, pl.ds(c * QUAD + t, L, stride=8), :] for t in range(QUAD)]
            for c in range(2)
        ]
        waves = jnp.concatenate([jnp.concatenate(part, 1) for part in tiles], 0)
        cells = right_table(waves, zb, ((0,), (0,)))
        cells = jnp.exp(0.5 * cells)
        start = f * 4 * CY * 2
        for t in range(QUAD):
            xs, ys = quarter(t)
            block = cells[tile(t)].reshape(8, 16, LZ)
            mod_ref[f, xs, ys, :] = block
            half_x = block.reshape(4, 2, 16, LZ)
            half_x = half_x[:, 0] + half_x[:, 1]
            for x in range(4):
                fold(start + ((t // 2) * 4 + x) * CY + (t % 2) * 16, half_x[x])
        stored = pltpu.make_async_copy(mod_ref.at[f], mod_out.at[f], fetch_sems.at[len(fetches) + f])
        stored.start()
        rows_one = pair_rows(start, 8 * 16)
        one = z_pool(rows_one, slice(0, 128))
        for i in range(PY):
            one_send[f, i] = one[i * 8 : i * 8 + 8]
        return stored, rows_one, across(one_send.at[f], (one_recv_0, one_recv_1)[f], 7 + f * PY)

    def choose(source, target, pieces):
        for g in range(PY):
            for level, rows in pieces:
                target[g, rows, :] = source[group_ref[level, g], rows, :]

    landed(back_send.at[0], back_recv.at[0], 8, 3)
    stored_0, rows_0, one_0 = coarse(0)
    landed(back_send.at[1], back_recv.at[1], 8, 4)
    stored_1, rows_1, one_1 = coarse(1)
    rows_one = jnp.concatenate([rows_0, rows_1], 0)
    pairs = rows_one.reshape(2 * 4, 2, 16, LZ)
    fold(0, (pairs[:, 0] + pairs[:, 1]).reshape(2 * 4 * 16, LZ))
    rows_two = pair_rows(0, 2 * 4 * 8)
    pairs = rows_two.reshape(2 * 2, 2, 8, LZ)
    fold(0, (pairs[:, 0] + pairs[:, 1]).reshape(2 * 2 * 8, LZ))
    rows_three = pair_rows(0, 2 * 2 * 4)
    rest = z_pool(jnp.concatenate([rows_two, rows_three], 0), slice(128, 256))
    for i in range(PY):
        rest_send[i, pl.ds(0, 4), :] = rest[i * 4 : i * 4 + 4]
        rest_send[i, pl.ds(4, 1), :] = rest[64 + i : 65 + i]
        rest_send[i, pl.ds(5, 3), :] = jnp.zeros((3, L), F32)
        rest_back[i, pl.ds(5, 3), :] = jnp.zeros((3, L), F32)
    rest_0 = across(rest_send, rest_recv, 7 + 2 * PY)
    for copy in one_0:
        copy.wait()
    choose(one_recv_0, one_back.at[0], [(0, pl.ds(0, 8))])
    last = across(one_back.at[0], one_out.at[0], 7 + 3 * PY)
    for copy in one_1:
        copy.wait()
    choose(one_recv_1, one_back.at[1], [(0, pl.ds(0, 8))])
    last += across(one_back.at[1], one_out.at[1], 7 + 4 * PY)
    for copy in rest_0:
        copy.wait()
    choose(rest_recv, rest_back, [(1, pl.ds(0, 4)), (2, pl.ds(4, 1))])
    last += across(rest_back, rest_out, 7 + 5 * PY)
    for copy in last:
        copy.wait()
    stored_0.wait()
    stored_1.wait()


def store_kernel(
    mod_in, one_in, rest_in, mod_out, one_out, two_out, three_out,
    mod_ref, one_held, rest_held, one_ref, two_ref, three_ref, in_sems, out_sems,
):
    pairs = [(mod_in.at[f, pl.ds(h * 8, 8)], mod_ref.at[f, pl.ds(h * 8, 8)]) for f in range(2) for h in range(2)]
    pairs += [(one_in, one_held), (rest_in, rest_held)]
    outs = [(mod_ref.at[f, pl.ds(h * 8, 8)], mod_out.at[f, pl.ds(h * 8, 8)]) for f in range(2) for h in range(2)]
    outs += [(one_ref, one_out), (two_ref, two_out), (three_ref, three_out)]
    loads = [pltpu.make_async_copy(*pair, in_sems.at[i]) for i, pair in enumerate(pairs)]
    stores = [pltpu.make_async_copy(*pair, out_sems.at[i]) for i, pair in enumerate(outs)]
    for load in loads[4:] + loads[:4]:
        load.start()
    loads[4].wait()
    loads[5].wait()
    for f in range(2):
        one_ref[f] = one_held[f].reshape(8, 16, L)
        for x in range(4):
            for h in range(2):
                two_ref[f, x, pl.ds(h * 4, 4), :] = rest_held[(f * 4 + x) * 2 + h, pl.ds(0, 4), :][:, :64]
        for x in range(2):
            for y in range(4):
                row = rest_held[(f * 2 + x) * 4 + y, pl.ds(4, 1), :]
                three_ref[f, x, pl.ds(y, 1), :] = row[:, 64:96]
    for store in stores[4:]:
        store.start()
    for i in range(4):
        loads[i].wait()
        stores[i].start()
    for store in stores:
        store.wait()


def on_device(white_noise, spectrum, group_table):
    shapes = [
        white_noise.shape,
        (2, CX // 2, CY // 2, LZ // 2),
        (2, CX // 4, CY // 4, LZ // 4),
        (2, CX // 8, CY // 8, LZ // 8),
    ]
    hbm = pl.BlockSpec(memory_space=pltpu.HBM)
    wide = pltpu.VMEM((2, DEV * 8, L), F32)
    thin = pltpu.VMEM((DEV * QUAD, L), F32)
    table = pltpu.VMEM((QUAD, L, L), F32)
    one, rest = (2, PY, 8, L), (PY, 8, L)
    slots = 7 + 6 * PY
    operands = [white_noise, spectrum] + tables()
    results = pl.pallas_call(
        kernel,
        out_shape=[jax.ShapeDtypeStruct(shape, F32) for shape in (shapes[0], one, rest)],
        in_specs=[hbm] * (len(operands) + 1),
        out_specs=[hbm] * 3,
        scratch_shapes=[pltpu.SMEM(group_table.shape, jnp.int32)]
        + [pltpu.VMEM(value.shape, value.dtype) for value in operands]
        + [thin, thin, pltpu.VMEM((QUAD, L), F32)]
        + [pltpu.VMEM((size, QUAD, L), F32) for size in (PY, DEV)]
        + [table, table, wide, wide, wide, wide]
        + [pltpu.VMEM(shapes[0], F32), pltpu.VMEM((2, 2 * 8 * CY, L), F32)]
        + [pltpu.VMEM(shape, F32) for shape in (one, rest, rest, one, rest, rest, rest)]
        + [pltpu.SemaphoreType.DMA((size,)) for size in (len(operands) + 3, slots, slots, slots)],
        compiler_params=pltpu.CompilerParams(
            collective_id=0, has_side_effects=True, vmem_limit_bytes=67_043_328
        ),
    )(group_table, *operands)
    return pl.pallas_call(
        store_kernel,
        out_shape=[jax.ShapeDtypeStruct(shape, F32) for shape in shapes],
        in_specs=[hbm] * 3,
        out_specs=[hbm] * 4,
        scratch_shapes=[pltpu.VMEM(shape, F32) for shape in (shapes[0], one, rest, *shapes[1:])]
        + [pltpu.SemaphoreType.DMA((8,)), pltpu.SemaphoreType.DMA((8,))],
        compiler_params=pltpu.CompilerParams(vmem_limit_bytes=67_043_328),
    )(*results)


def solution(mesh):
    in_specs = (P(None, "px", "py", None), P("px", "py", None), P())
    out_specs = (P(None, "px", "py", None),) * 4
    return jax.shard_map(
        on_device, mesh=mesh, in_specs=in_specs, out_specs=out_specs, check_vma=False
    )
```

```python
import numpy as np

import jax
import jax.numpy as jnp
from jax import lax
from jax.experimental import pallas as pl
from jax.experimental.pallas import tpu as pltpu
from jax.sharding import PartitionSpec as P

MESH = pl.DeviceIdType.MESH
F32, BF16 = jnp.float32, jnp.bfloat16
PX, PY = 8, 16
DEV = PX * PY
LX, LY, LZ = 128, 512, 256
CX, CY = LX // PX, LY // PY
L = 128
QUAD = 4


def split(values):
    values = np.asarray(values, np.float32)
    high = values.astype(jnp.bfloat16)
    low = (values - high.astype(np.float32)).astype(jnp.bfloat16)
    return np.stack([high, low], 0)


def tables():
    k = np.arange(L)
    z = np.arange(LZ)
    angle = 2.0 * np.pi / LZ * (k[:, None] * z[None, :] % LZ)
    nyquist = np.where(z % 2 == 0, 1.0, -1.0)
    ahead = np.stack([np.cos(angle), -np.sin(angle)], 0)
    back = 2.0 * ahead
    ahead[1, 0] = nyquist
    back[0, 0] = 1.0
    back[1, 0] = nyquist
    z_ahead = split(ahead.reshape(LZ, LZ))
    z_back = split(back.reshape(LZ, LZ) / (LX * LY * LZ))
    first, second = k // 16, k % 16
    turn = first[:, None] * first[None, :] / 8.0 + second[:, None] * second[None, :] / 16.0
    cos, sin = np.cos(2 * np.pi * turn), -np.sin(2 * np.pi * turn)
    column = split(np.block([[cos, -sin], [sin, cos]]))
    row = split(np.block([[cos, sin], [-sin, cos]]))
    twiddle, small = [], []
    for t in range(QUAD):
        xl = (t // 2) * 8 + first
        yl = (t % 2) * 16 + second
        turn = first[:, None] * xl[None, :] / LX + second[:, None] * yl[None, :] / LY
        twiddle.append(np.stack([np.cos(2 * np.pi * turn), -np.sin(2 * np.pi * turn)], 0))
        turn = (t // 2) * first / 16.0 + (t % 2) * second / 32.0
        small.append(np.stack([np.cos(2 * np.pi * turn), -np.sin(2 * np.pi * turn)], 0))
    twiddle = np.concatenate(twiddle, 2).astype(np.float32)
    small = np.stack(small, 1).reshape(2 * QUAD, L).astype(np.float32)
    pool = np.zeros((LZ, LZ))
    pool[z, z // 2] = 1.0 / 8
    pool[z, 128 + z // 4] = 1.0 / 64
    pool[z, 192 + z // 8] = 1.0 / 512
    return [
        jnp.asarray(v)
        for v in (z_ahead, z_back, column, row, twiddle, small, pool.astype(jnp.bfloat16))
    ]


def parts(values):
    high = values.astype(BF16)
    return high, (values - high.astype(F32)).astype(BF16)


def product(left, right, dims):
    return lax.dot_general(left, right, (dims, ((), ())), preferred_element_type=F32)


def left_table(table, values, dims=((1,), (0,))):
    high, low = parts(values)
    first = product(table[0], high, dims) + product(table[0], low, dims)
    return first + product(table[1], high, dims)


def right_table(values, table, dims=((1,), (0,))):
    high, low = parts(values)
    first = product(high, table[0], dims) + product(low, table[0], dims)
    return first + product(high, table[1], dims)


def hops(shift):
    return sum(min(d, 4 - d) for d in shift[:3])


SHIFTS = [(dz, dy, dx, dc) for dz in range(4) for dy in range(4) for dx in range(4) for dc in range(2)]
MIXED = [SHIFTS[(i * 37) % 128] for i in range(1, 128)]
SHIFTS = sorted(SHIFTS[1:], key=lambda shift: -hops(shift))

LINE = [(dx, low) for dx in range(4) for low in range(4)]
LINE = sorted(LINE[1:], key=lambda move: -min(move[0], 4 - move[0]) - (move[1] >> 1))


def place():
    px, py = lax.axis_index("px"), lax.axis_index("py")
    return (px >> 2) * 2 + ((py >> 1) & 1), px & 3, py >> 2, py & 1


def shifted(here, dz, dy, dx, dc):
    z, y, x = ((here[i] + d) & 3 for i, d in enumerate((dz, dy, dx)))
    px = (z >> 1) * 4 + y
    py = x * 4 + (z & 1) * 2 + (here[3] ^ dc)
    return px * PY + py, {"px": px, "py": py}


def quarter(t):
    return slice((t // 2) * 8, (t // 2) * 8 + 8), slice((t % 2) * 16, (t % 2) * 16 + 16)


def tile(t):
    return slice(t * L, (t + 1) * L)


def butterfly(values):
    a, b, c, d = values
    p, q, r, s = a + b, a - b, c + d, c - d
    return [p + r, q + s, p - r, q - s]


def turned(real, imag, cos, sin):
    return real * cos - imag * sin, real * sin + imag * cos


def piece(index, height):
    return pl.ds(pl.multiple_of(index * height, height), height)


def kernel(
    group_in, noise_in, spec_in, za_in, zb_in, col_in, row_in, tw_in, small_in, pool_in,
    mod_out, one_out, rest_out,
    group_ref, noise_ref, spec_ref, za_ref, zb_ref, col_ref, row_ref, tw_ref, small_ref, pool_ref,
    s_send, s_recv, n_send, n_line, n_recv, u_table, v_table, ahead_send, ahead_recv, back_send, back_recv,
    mod_ref, half_y, one_send, one_recv_0, one_recv_1, one_back, rest_send, rest_recv, rest_back,
    fetch_sems, local_sems, send_sems, recv_sems,
):
    here = place()
    my_px, my_py = lax.axis_index("px"), lax.axis_index("py")
    me = my_px * PY + my_py
    barrier = pltpu.get_barrier_semaphore()

    pairs = (
        (spec_in, spec_ref), (noise_in, noise_ref), (za_in, za_ref), (col_in, col_ref),
        (row_in, row_ref), (tw_in, tw_ref), (small_in, small_ref), (zb_in, zb_ref),
        (pool_in, pool_ref), (group_in, group_ref),
    )
    fetches = [
        pltpu.make_async_copy(source, target, fetch_sems.at[index])
        for index, (source, target) in enumerate(pairs)
    ]
    for fetch in fetches:
        fetch.start()

    for shift in SHIFTS:
        pl.semaphore_signal(barrier, inc=1, device_id=shifted(here, *shift)[1], device_id_type=MESH)

    def spread(send, recv, height, slot, order=MIXED):
        pltpu.make_async_copy(
            send.at[piece(me, height)], recv.at[piece(me, height)], local_sems.at[slot]
        ).start()

        def send_to(shift):
            other, device = shifted(here, *shift)
            pltpu.make_async_remote_copy(
                src_ref=send.at[piece(other, height)],
                dst_ref=recv.at[piece(me, height)],
                send_sem=send_sems.at[slot],
                recv_sem=recv_sems.at[slot],
                device_id=device,
                device_id_type=MESH,
            ).start()

        for shift in order:
            send_to(shift)

    def landed(send, recv, height, slot):
        pltpu.make_async_copy(
            send.at[piece(me, height)], recv.at[piece(me, height)], local_sems.at[slot]
        ).wait()
        rest = pl.ds(0, (DEV - 1) * height)
        whole = pltpu.make_async_remote_copy(
            src_ref=send.at[rest],
            dst_ref=recv.at[rest],
            send_sem=send_sems.at[slot],
            recv_sem=recv_sems.at[slot],
            device_id=shifted(here, 0, 0, 0, 1)[1],
            device_id_type=MESH,
        )
        whole.wait()

    fetches[0].wait()
    for t in range(QUAD):
        xs, ys = quarter(t)
        block = spec_ref[xs, ys, :].reshape(L, LZ)
        s_send[pl.ds(t, L, stride=QUAD), :] = block[:, :L].T
        n_send[pl.ds(t, 1), :] = block[:, L:].T[:1]

    fetches[1].wait()
    fetches[2].wait()
    za = (za_ref[0], za_ref[1])

    def z_ahead(f):
        rows = [noise_ref[(f,) + quarter(t)].reshape(L, LZ) for t in range(QUAD)]
        return left_table(za, jnp.concatenate(rows, 0), ((1,), (1,)))

    values = [z_ahead(0), z_ahead(1)]
    at_zero = lax.broadcasted_iota(jnp.int32, (L, QUAD * L), 0) == 0
    real_one = jnp.where(at_zero, values[0][L:], values[1][:L])
    imag_zero = jnp.where(at_zero, values[1][:L], values[0][L:])
    members = ((values[0][:L], imag_zero), (real_one, values[1][L:]))
    for f in range(2):
        for c in range(2):
            for t in range(QUAD):
                ahead_send[f, pl.ds(c * QUAD + t, L, stride=8), :] = members[f][c][:, tile(t)]

    pl.semaphore_wait(barrier, DEV - 1)
    line_copy = pltpu.make_async_remote_copy(
        src_ref=n_send,
        dst_ref=n_line.at[my_py],
        send_sem=send_sems.at[5],
        recv_sem=recv_sems.at[5],
        device_id={"py": 0},
        device_id_type=MESH,
    )
    plane_copies = [
        pltpu.make_async_remote_copy(
            src_ref=n_line.at[i],
            dst_ref=n_recv.at[my_px * PY + i],
            send_sem=send_sems.at[6],
            recv_sem=recv_sems.at[6],
            device_id={"px": 0},
            device_id_type=MESH,
        )
        for i in range(PY)
    ]

    def line_rest(device):
        rest = n_line.at[pl.ds(1, PY - 1)]
        return pltpu.make_async_remote_copy(
            src_ref=rest, dst_ref=rest, send_sem=send_sems.at[5], recv_sem=recv_sems.at[5],
            device_id=device, device_id_type=MESH,
        )

    def plane_rest(rest, device):
        return pltpu.make_async_remote_copy(
            src_ref=rest, dst_ref=rest, send_sem=send_sems.at[6], recv_sem=recv_sems.at[6],
            device_id=device, device_id_type=MESH,
        )

    pl.when(my_py != 0)(line_copy.start)
    spread(s_send, s_recv, QUAD, 0)

    spread(ahead_send.at[0], ahead_recv.at[0], 8, 1)

    @pl.when(my_py == 0)
    def _():
        n_line[0] = n_send[...]
        line_rest({"py": 1}).wait_recv()

        @pl.when(my_px != 0)
        def _():
            for copy in plane_copies:
                copy.start()

    spread(ahead_send.at[1], ahead_recv.at[1], 8, 2)

    landed(s_send, s_recv, QUAD, 0)
    for t in range(QUAD):
        u_table[t] = s_recv[pl.ds(t, L, stride=QUAD), :].T

    pl.when(my_py != 0)(line_copy.wait_send)
    for index in range(3, 7):
        fetches[index].wait()

    def last_table():
        @pl.when(me != 0)
        def _():
            v_table[...] = u_table[...]

        @pl.when((my_py == 0) & (my_px != 0))
        def _():
            plane_rest(n_line, {"px": 0}).wait_send()

        @pl.when(me == 0)
        def _():
            n_recv[pl.ds(0, PY)] = n_line[...]
            plane_rest(n_recv.at[pl.ds(PY, DEV - PY)], {"px": 1}).wait_recv()
            for t in range(QUAD):
                v_table[t] = n_recv[:, t, :].T

    column = (col_ref[0], col_ref[1])
    row = (row_ref[0], row_ref[1])
    for f in range(2):
        landed(ahead_send.at[f], ahead_recv.at[f], 8, 1 + f)
        if f == 1:
            last_table()
        plane = [
            jnp.concatenate(
                [ahead_recv[f, pl.ds(c * QUAD + t, L, stride=8), :] for t in range(QUAD)], 1
            )
            for c in range(2)
        ]
        mixed = left_table(column, jnp.concatenate(plane, 0))
        real, imag = turned(mixed[:L], mixed[L:], tw_ref[0], tw_ref[1])
        reals = butterfly([real[:, tile(t)] for t in range(QUAD)])
        imags = butterfly([imag[:, tile(t)] for t in range(QUAD)])
        rows = []
        for t in range(QUAD):
            cos, sin = small_ref[pl.ds(t, 1), :], small_ref[pl.ds(QUAD + t, 1), :]
            pair = turned(reals[t], imags[t], cos, sin) if t else (reals[t], imags[t])
            rows.append(jnp.concatenate(pair, 1))
        freq = right_table(jnp.concatenate(rows, 0), row)
        table = u_table if f == 0 else v_table
        scale = jnp.concatenate([table[t] for t in range(QUAD)], 0)
        freq = freq * jnp.concatenate([scale, scale], 1)
        mixed = right_table(freq, column)
        reals, imags = [], []
        for t in range(QUAD):
            part = mixed[tile(t)]
            pair = (part[:, :L], part[:, L:])
            if t:
                cos, sin = small_ref[pl.ds(t, 1), :], small_ref[pl.ds(QUAD + t, 1), :]
                pair = turned(*pair, cos, -sin)
            reals.append(pair[0])
            imags.append(pair[1])
        real = jnp.concatenate(butterfly(reals), 1)
        imag = jnp.concatenate(butterfly(imags), 1)
        real, imag = turned(real, imag, tw_ref[0], -tw_ref[1])
        plane = left_table(row, jnp.concatenate([real, imag], 0))
        for c in range(2):
            for t in range(QUAD):
                back_send[f, pl.ds(c * QUAD + t, L, stride=8), :] = plane[tile(c), tile(t)]
        if f == 0:
            pl.when(me != 0)(lambda: spread(back_send.at[0], back_recv.at[0], 8, 3, SHIFTS))
        else:

            @pl.when(me == 0)
            def _():
                for t in range(QUAD):
                    first, second = pl.ds(QUAD + t, L, stride=8), pl.ds(t, L, stride=8)
                    held = back_send[0, first, :], back_send[1, second, :]
                    back_send[0, first, :], back_send[1, second, :] = held[1], held[0]
                spread(back_send.at[0], back_recv.at[0], 8, 3, SHIFTS)

            spread(back_send.at[1], back_recv.at[1], 8, 4, SHIFTS)

    for index in range(7, 10):
        fetches[index].wait()
    zb = (zb_ref[0], zb_ref[1])

    def fold(start, rows):
        for h in range(2):
            half_y[h, pl.ds(start, rows.shape[0]), :] = rows[:, tile(h)]

    def pair_rows(start, count):
        rows = [
            half_y[h, pl.ds(start, count, stride=2), :] + half_y[h, pl.ds(start + 1, count, stride=2), :]
            for h in range(2)
        ]
        return jnp.concatenate(rows, 1)

    def z_pool(values, lanes):
        high, low = parts(values)
        pool = pool_ref[:, lanes]
        return product(high, pool, ((1,), (0,))) + product(low, pool, ((1,), (0,)))

    def across(send, recv, slot):
        own = pltpu.make_async_copy(send.at[my_py], recv.at[my_py], local_sems.at[slot])
        own.start()
        for dx, low in LINE:
            other = (((my_py >> 2) + dx) & 3) * 4 + ((my_py & 3) ^ low)
            pltpu.make_async_remote_copy(
                src_ref=send.at[other],
                dst_ref=recv.at[my_py],
                send_sem=send_sems.at[slot],
                recv_sem=recv_sems.at[slot],
                device_id={"py": other},
                device_id_type=MESH,
            ).start()
        rest = pl.ds(0, PY - 1)
        whole = pltpu.make_async_remote_copy(
            src_ref=send.at[rest],
            dst_ref=recv.at[rest],
            send_sem=send_sems.at[slot],
            recv_sem=recv_sems.at[slot],
            device_id={"py": my_py ^ 1},
            device_id_type=MESH,
        )
        return [own, whole]

    def coarse(f):
        tiles = [
            [back_recv[f, pl.ds(c * QUAD + t, L, stride=8), :] for t in range(QUAD)]
            for c in range(2)
        ]
        waves = jnp.concatenate([jnp.concatenate(part, 1) for part in tiles], 0)
        cells = right_table(waves, zb, ((0,), (0,)))
        cells = jnp.exp(0.5 * cells)
        start = f * 4 * CY * 2
        for t in range(QUAD):
            xs, ys = quarter(t)
            block = cells[tile(t)].reshape(8, 16, LZ)
            mod_ref[f, xs, ys, :] = block
            half_x = block.reshape(4, 2, 16, LZ)
            half_x = half_x[:, 0] + half_x[:, 1]
            for x in range(4):
                fold(start + ((t // 2) * 4 + x) * CY + (t % 2) * 16, half_x[x])
        stored = pltpu.make_async_copy(mod_ref.at[f], mod_out.at[f], fetch_sems.at[len(fetches) + f])
        stored.start()
        rows_one = pair_rows(start, 8 * 16)
        one = z_pool(rows_one, slice(0, 128))
        for i in range(PY):
            one_send[f, i] = one[i * 8 : i * 8 + 8]
        return stored, rows_one, across(one_send.at[f], (one_recv_0, one_recv_1)[f], 7 + f)

    def choose(source, target, pieces):
        for g in range(PY):
            for level, rows in pieces:
                target[g, rows, :] = source[group_ref[level, g], rows, :]

    landed(back_send.at[0], back_recv.at[0], 8, 3)
    stored_0, rows_0, one_0 = coarse(0)
    landed(back_send.at[1], back_recv.at[1], 8, 4)
    stored_1, rows_1, one_1 = coarse(1)
    rows_one = jnp.concatenate([rows_0, rows_1], 0)
    pairs = rows_one.reshape(2 * 4, 2, 16, LZ)
    fold(0, (pairs[:, 0] + pairs[:, 1]).reshape(2 * 4 * 16, LZ))
    rows_two = pair_rows(0, 2 * 4 * 8)
    pairs = rows_two.reshape(2 * 2, 2, 8, LZ)
    fold(0, (pairs[:, 0] + pairs[:, 1]).reshape(2 * 2 * 8, LZ))
    rows_three = pair_rows(0, 2 * 2 * 4)
    rest = z_pool(jnp.concatenate([rows_two, rows_three], 0), slice(128, 256))
    for i in range(PY):
        rest_send[i, pl.ds(0, 4), :] = rest[i * 4 : i * 4 + 4]
        rest_send[i, pl.ds(4, 1), :] = rest[64 + i : 65 + i]
        rest_send[i, pl.ds(5, 3), :] = jnp.zeros((3, L), F32)
        rest_back[i, pl.ds(5, 3), :] = jnp.zeros((3, L), F32)
    rest_0 = across(rest_send, rest_recv, 9)
    for copy in one_0:
        copy.wait()
    choose(one_recv_0, one_back.at[0], [(0, pl.ds(0, 8))])
    last = across(one_back.at[0], one_out.at[0], 10)
    for copy in one_1:
        copy.wait()
    choose(one_recv_1, one_back.at[1], [(0, pl.ds(0, 8))])
    last += across(one_back.at[1], one_out.at[1], 11)
    for copy in rest_0:
        copy.wait()
    choose(rest_recv, rest_back, [(1, pl.ds(0, 4)), (2, pl.ds(4, 1))])
    last += across(rest_back, rest_out, 12)
    for copy in last:
        copy.wait()
    stored_0.wait()
    stored_1.wait()


def store_kernel(
    mod_in, one_in, rest_in, mod_out, one_out, two_out, three_out,
    mod_ref, one_held, rest_held, one_ref, two_ref, three_ref, in_sems, out_sems,
):
    pairs = [(mod_in.at[f, pl.ds(h * 8, 8)], mod_ref.at[f, pl.ds(h * 8, 8)]) for f in range(2) for h in range(2)]
    pairs += [(one_in, one_held), (rest_in, rest_held)]
    outs = [(mod_ref.at[f, pl.ds(h * 8, 8)], mod_out.at[f, pl.ds(h * 8, 8)]) for f in range(2) for h in range(2)]
    outs += [(one_ref, one_out), (two_ref, two_out), (three_ref, three_out)]
    loads = [pltpu.make_async_copy(*pair, in_sems.at[i]) for i, pair in enumerate(pairs)]
    stores = [pltpu.make_async_copy(*pair, out_sems.at[i]) for i, pair in enumerate(outs)]
    for load in loads[4:] + loads[:4]:
        load.start()
    loads[4].wait()
    loads[5].wait()
    for f in range(2):
        one_ref[f] = one_held[f].reshape(8, 16, L)
        for x in range(4):
            for h in range(2):
                two_ref[f, x, pl.ds(h * 4, 4), :] = rest_held[(f * 4 + x) * 2 + h, pl.ds(0, 4), :][:, :64]
        for x in range(2):
            for y in range(4):
                row = rest_held[(f * 2 + x) * 4 + y, pl.ds(4, 1), :]
                three_ref[f, x, pl.ds(y, 1), :] = row[:, 64:96]
    for store in stores[4:]:
        store.start()
    for i in range(4):
        loads[i].wait()
        stores[i].start()
    for store in stores:
        store.wait()


def on_device(white_noise, spectrum, group_table):
    shapes = [
        white_noise.shape,
        (2, CX // 2, CY // 2, LZ // 2),
        (2, CX // 4, CY // 4, LZ // 4),
        (2, CX // 8, CY // 8, LZ // 8),
    ]
    hbm = pl.BlockSpec(memory_space=pltpu.HBM)
    wide = pltpu.VMEM((2, DEV * 8, L), F32)
    thin = pltpu.VMEM((DEV * QUAD, L), F32)
    table = pltpu.VMEM((QUAD, L, L), F32)
    one, rest = (2, PY, 8, L), (PY, 8, L)
    slots = 13
    operands = [white_noise, spectrum] + tables()
    results = pl.pallas_call(
        kernel,
        out_shape=[jax.ShapeDtypeStruct(shape, F32) for shape in (shapes[0], one, rest)],
        in_specs=[hbm] * (len(operands) + 1),
        out_specs=[hbm] * 3,
        scratch_shapes=[pltpu.SMEM(group_table.shape, jnp.int32)]
        + [pltpu.VMEM(value.shape, value.dtype) for value in operands]
        + [thin, thin, pltpu.VMEM((QUAD, L), F32)]
        + [pltpu.VMEM((size, QUAD, L), F32) for size in (PY, DEV)]
        + [table, table, wide, wide, wide, wide]
        + [pltpu.VMEM(shapes[0], F32), pltpu.VMEM((2, 2 * 8 * CY, L), F32)]
        + [pltpu.VMEM(shape, F32) for shape in (one, rest, rest, one, rest, rest, rest)]
        + [pltpu.SemaphoreType.DMA((size,)) for size in (len(operands) + 3, slots, slots, slots)],
        compiler_params=pltpu.CompilerParams(
            collective_id=0, has_side_effects=True, vmem_limit_bytes=67_043_328
        ),
    )(group_table, *operands)
    return pl.pallas_call(
        store_kernel,
        out_shape=[jax.ShapeDtypeStruct(shape, F32) for shape in shapes],
        in_specs=[hbm] * 3,
        out_specs=[hbm] * 4,
        scratch_shapes=[pltpu.VMEM(shape, F32) for shape in (shapes[0], one, rest, *shapes[1:])]
        + [pltpu.SemaphoreType.DMA((8,)), pltpu.SemaphoreType.DMA((8,))],
        compiler_params=pltpu.CompilerParams(vmem_limit_bytes=67_043_328),
    )(*results)


def solution(mesh):
    in_specs = (P(None, "px", "py", None), P("px", "py", None), P())
    out_specs = (P(None, "px", "py", None),) * 4
    return jax.shard_map(
        on_device, mesh=mesh, in_specs=in_specs, out_specs=out_specs, check_vma=False
    )
```

```python
import numpy as np

import jax
import jax.numpy as jnp
from jax import lax
from jax.experimental import pallas as pl
from jax.experimental.pallas import tpu as pltpu
from jax.sharding import PartitionSpec as P

MESH = pl.DeviceIdType.MESH
F32, BF16 = jnp.float32, jnp.bfloat16
PX, PY = 8, 16
DEV = PX * PY
LX, LY, LZ = 128, 512, 256
CX, CY = LX // PX, LY // PY
L = 128
QUAD = 4


def split(values):
    values = np.asarray(values, np.float32)
    high = values.astype(jnp.bfloat16)
    low = (values - high.astype(np.float32)).astype(jnp.bfloat16)
    return np.stack([high, low], 0)


def tables():
    k = np.arange(L)
    z = np.arange(LZ)
    angle = 2.0 * np.pi / LZ * (k[:, None] * z[None, :] % LZ)
    nyquist = np.where(z % 2 == 0, 1.0, -1.0)
    ahead = np.stack([np.cos(angle), -np.sin(angle)], 0)
    back = 2.0 * ahead
    ahead[1, 0] = nyquist
    back[0, 0] = 1.0
    back[1, 0] = nyquist
    z_ahead = split(ahead.reshape(LZ, LZ))
    z_back = split(back.reshape(LZ, LZ) / (LX * LY * LZ))
    first, second = k // 16, k % 16
    turn = first[:, None] * first[None, :] / 8.0 + second[:, None] * second[None, :] / 16.0
    cos, sin = np.cos(2 * np.pi * turn), -np.sin(2 * np.pi * turn)
    column = split(np.block([[cos, -sin], [sin, cos]]))
    row = split(np.block([[cos, sin], [-sin, cos]]))
    twiddle, small = [], []
    for t in range(QUAD):
        xl = (t // 2) * 8 + first
        yl = (t % 2) * 16 + second
        turn = first[:, None] * xl[None, :] / LX + second[:, None] * yl[None, :] / LY
        twiddle.append(np.stack([np.cos(2 * np.pi * turn), -np.sin(2 * np.pi * turn)], 0))
        turn = (t // 2) * first / 16.0 + (t % 2) * second / 32.0
        small.append(np.stack([np.cos(2 * np.pi * turn), -np.sin(2 * np.pi * turn)], 0))
    twiddle = np.concatenate(twiddle, 2).astype(np.float32)
    small = np.stack(small, 1).reshape(2 * QUAD, L).astype(np.float32)
    pool = np.zeros((LZ, LZ))
    pool[z, z // 2] = 1.0 / 8
    pool[z, 128 + z // 4] = 1.0 / 64
    pool[z, 192 + z // 8] = 1.0 / 512
    return [
        jnp.asarray(v)
        for v in (z_ahead, z_back, column, row, twiddle, small, pool.astype(jnp.bfloat16))
    ]


def parts(values):
    high = values.astype(BF16)
    return high, (values - high.astype(F32)).astype(BF16)


def product(left, right, dims):
    return lax.dot_general(left, right, (dims, ((), ())), preferred_element_type=F32)


def left_table(table, values, dims=((1,), (0,))):
    high, low = parts(values)
    first = product(table[0], high, dims) + product(table[0], low, dims)
    return first + product(table[1], high, dims)


def right_table(values, table, dims=((1,), (0,))):
    high, low = parts(values)
    first = product(high, table[0], dims) + product(low, table[0], dims)
    return first + product(high, table[1], dims)


def hops(shift):
    return sum(min(d, 4 - d) for d in shift[:3])


SHIFTS = [(dz, dy, dx, dc) for dz in range(4) for dy in range(4) for dx in range(4) for dc in range(2)]


def spread_evenly(shifts):
    load = np.zeros(6)
    order, left = [], list(shifts)
    while left:
        def cost(shift):
            after = load.copy()
            for axis, d in enumerate(shift[:3]):
                after[2 * axis] += (0, 1, 1, 0)[d]
                after[2 * axis + 1] += (0, 0, 1, 1)[d]
            return after.max() - after.min()
        best = min(left, key=cost)
        for axis, d in enumerate(best[:3]):
            load[2 * axis] += (0, 1, 1, 0)[d]
            load[2 * axis + 1] += (0, 0, 1, 1)[d]
        left.remove(best)
        order.append(best)
    return order


MIXED = spread_evenly([SHIFTS[(i * 37) % 128] for i in range(1, 128)])
SHIFTS = sorted(SHIFTS[1:], key=lambda shift: -hops(shift))

LINE = [(dx, low) for dx in range(4) for low in range(4)]
LINE = sorted(LINE[1:], key=lambda move: -min(move[0], 4 - move[0]) - (move[1] >> 1))


def place():
    px, py = lax.axis_index("px"), lax.axis_index("py")
    return (px >> 2) * 2 + ((py >> 1) & 1), px & 3, py >> 2, py & 1


def shifted(here, dz, dy, dx, dc):
    z, y, x = ((here[i] + d) & 3 for i, d in enumerate((dz, dy, dx)))
    px = (z >> 1) * 4 + y
    py = x * 4 + (z & 1) * 2 + (here[3] ^ dc)
    return px * PY + py, {"px": px, "py": py}


def quarter(t):
    return slice((t // 2) * 8, (t // 2) * 8 + 8), slice((t % 2) * 16, (t % 2) * 16 + 16)


def tile(t):
    return slice(t * L, (t + 1) * L)


def butterfly(values):
    a, b, c, d = values
    p, q, r, s = a + b, a - b, c + d, c - d
    return [p + r, q + s, p - r, q - s]


def turned(real, imag, cos, sin):
    return real * cos - imag * sin, real * sin + imag * cos


def piece(index, height):
    return pl.ds(pl.multiple_of(index * height, height), height)


def kernel(
    group_in, noise_in, spec_in, za_in, zb_in, col_in, row_in, tw_in, small_in, pool_in,
    mod_out, one_out, rest_out,
    group_ref, noise_ref, spec_ref, za_ref, zb_ref, col_ref, row_ref, tw_ref, small_ref, pool_ref,
    s_send, s_recv, n_send, n_line, n_recv, u_table, v_table, ahead_send, ahead_recv, back_send, back_recv, zero_send,
    mod_ref, half_y, one_send, one_recv_0, one_recv_1, one_back, rest_send, rest_recv, rest_back,
    fetch_sems, local_sems, send_sems, recv_sems,
):
    here = place()
    my_px, my_py = lax.axis_index("px"), lax.axis_index("py")
    me = my_px * PY + my_py
    barrier = pltpu.get_barrier_semaphore()

    pairs = (
        (spec_in, spec_ref), (noise_in, noise_ref), (za_in, za_ref), (col_in, col_ref),
        (row_in, row_ref), (tw_in, tw_ref), (small_in, small_ref), (zb_in, zb_ref),
        (pool_in, pool_ref), (group_in, group_ref),
    )
    fetches = [
        pltpu.make_async_copy(source, target, fetch_sems.at[index])
        for index, (source, target) in enumerate(pairs)
    ]
    for fetch in fetches:
        fetch.start()

    for shift in SHIFTS:
        pl.semaphore_signal(barrier, inc=1, device_id=shifted(here, *shift)[1], device_id_type=MESH)

    def spread(send, recv, height, slot, order=MIXED):
        pltpu.make_async_copy(
            send.at[piece(me, height)], recv.at[piece(me, height)], local_sems.at[slot]
        ).start()

        def send_to(shift):
            other, device = shifted(here, *shift)
            pltpu.make_async_remote_copy(
                src_ref=send.at[piece(other, height)],
                dst_ref=recv.at[piece(me, height)],
                send_sem=send_sems.at[slot],
                recv_sem=recv_sems.at[slot],
                device_id=device,
                device_id_type=MESH,
            ).start()

        for shift in order:
            send_to(shift)

    def landed(send, recv, height, slot, packed=False):
        own = pltpu.make_async_copy(
            send.at[piece(me, height)], recv.at[piece(me, height)], local_sems.at[slot]
        )
        if packed:
            pl.when(me != 0)(own.wait)
        else:
            own.wait()
        rest = pl.ds(0, (DEV - 1) * height)
        whole = pltpu.make_async_remote_copy(
            src_ref=send.at[rest],
            dst_ref=recv.at[rest],
            send_sem=send_sems.at[slot],
            recv_sem=recv_sems.at[slot],
            device_id=shifted(here, 0, 0, 0, 1)[1],
            device_id_type=MESH,
        )
        whole.wait()

    fetches[0].wait()
    for t in range(QUAD):
        xs, ys = quarter(t)
        block = spec_ref[xs, ys, :].reshape(L, LZ)
        s_send[pl.ds(t, L, stride=QUAD), :] = block[:, :L].T
        n_send[pl.ds(t, 1), :] = block[:, L:].T[:1]

    fetches[1].wait()
    fetches[2].wait()
    za = (za_ref[0], za_ref[1])

    def z_ahead(f):
        rows = [noise_ref[(f,) + quarter(t)].reshape(L, LZ) for t in range(QUAD)]
        return left_table(za, jnp.concatenate(rows, 0), ((1,), (1,)))

    values = [z_ahead(0), z_ahead(1)]
    at_zero = lax.broadcasted_iota(jnp.int32, (L, QUAD * L), 0) == 0
    real_one = jnp.where(at_zero, values[0][L:], values[1][:L])
    imag_zero = jnp.where(at_zero, values[1][:L], values[0][L:])
    members = ((values[0][:L], imag_zero), (real_one, values[1][L:]))
    for f in range(2):
        for c in range(2):
            for t in range(QUAD):
                ahead_send[f, pl.ds(c * QUAD + t, L, stride=8), :] = members[f][c][:, tile(t)]

    pl.semaphore_wait(barrier, DEV - 1)
    line_copy = pltpu.make_async_remote_copy(
        src_ref=n_send,
        dst_ref=n_line.at[my_py],
        send_sem=send_sems.at[5],
        recv_sem=recv_sems.at[5],
        device_id={"py": 0},
        device_id_type=MESH,
    )
    plane_copies = [
        pltpu.make_async_remote_copy(
            src_ref=n_line.at[i],
            dst_ref=n_recv.at[my_px * PY + i],
            send_sem=send_sems.at[6],
            recv_sem=recv_sems.at[6],
            device_id={"px": 0},
            device_id_type=MESH,
        )
        for i in range(PY)
    ]

    def line_rest(device):
        rest = n_line.at[pl.ds(1, PY - 1)]
        return pltpu.make_async_remote_copy(
            src_ref=rest, dst_ref=rest, send_sem=send_sems.at[5], recv_sem=recv_sems.at[5],
            device_id=device, device_id_type=MESH,
        )

    def plane_rest(rest, device):
        return pltpu.make_async_remote_copy(
            src_ref=rest, dst_ref=rest, send_sem=send_sems.at[6], recv_sem=recv_sems.at[6],
            device_id=device, device_id_type=MESH,
        )

    pl.when(my_py != 0)(line_copy.start)
    spread(s_send, s_recv, QUAD, 0)

    spread(ahead_send.at[0], ahead_recv.at[0], 8, 1)

    @pl.when(my_py == 0)
    def _():
        n_line[0] = n_send[...]
        line_rest({"py": 1}).wait_recv()

        @pl.when(my_px != 0)
        def _():
            for copy in plane_copies:
                copy.start()

    spread(ahead_send.at[1], ahead_recv.at[1], 8, 2, SHIFTS)

    landed(s_send, s_recv, QUAD, 0)
    for t in range(QUAD):
        u_table[t] = s_recv[pl.ds(t, L, stride=QUAD), :].T

    pl.when(my_py != 0)(line_copy.wait_send)
    for index in range(3, 7):
        fetches[index].wait()

    def last_table():
        @pl.when(me != 0)
        def _():
            v_table[...] = u_table[...]

        @pl.when((my_py == 0) & (my_px != 0))
        def _():
            plane_rest(n_line, {"px": 0}).wait_send()

        @pl.when(me == 0)
        def _():
            n_recv[pl.ds(0, PY)] = n_line[...]
            plane_rest(n_recv.at[pl.ds(PY, DEV - PY)], {"px": 1}).wait_recv()
            for t in range(QUAD):
                v_table[t] = n_recv[:, t, :].T

    column = (col_ref[0], col_ref[1])
    row = (row_ref[0], row_ref[1])
    for f in range(2):
        landed(ahead_send.at[f], ahead_recv.at[f], 8, 1 + f)
        if f == 1:
            last_table()
        plane = [
            jnp.concatenate(
                [ahead_recv[f, pl.ds(c * QUAD + t, L, stride=8), :] for t in range(QUAD)], 1
            )
            for c in range(2)
        ]
        mixed = left_table(column, jnp.concatenate(plane, 0))
        real, imag = turned(mixed[:L], mixed[L:], tw_ref[0], tw_ref[1])
        reals = butterfly([real[:, tile(t)] for t in range(QUAD)])
        imags = butterfly([imag[:, tile(t)] for t in range(QUAD)])
        rows = []
        for t in range(QUAD):
            cos, sin = small_ref[pl.ds(t, 1), :], small_ref[pl.ds(QUAD + t, 1), :]
            pair = turned(reals[t], imags[t], cos, sin) if t else (reals[t], imags[t])
            rows.append(jnp.concatenate(pair, 1))
        freq = right_table(jnp.concatenate(rows, 0), row)
        table = u_table if f == 0 else v_table
        scale = jnp.concatenate([table[t] for t in range(QUAD)], 0)
        freq = freq * jnp.concatenate([scale, scale], 1)
        mixed = right_table(freq, column)
        reals, imags = [], []
        for t in range(QUAD):
            part = mixed[tile(t)]
            pair = (part[:, :L], part[:, L:])
            if t:
                cos, sin = small_ref[pl.ds(t, 1), :], small_ref[pl.ds(QUAD + t, 1), :]
                pair = turned(*pair, cos, -sin)
            reals.append(pair[0])
            imags.append(pair[1])
        real = jnp.concatenate(butterfly(reals), 1)
        imag = jnp.concatenate(butterfly(imags), 1)
        real, imag = turned(real, imag, tw_ref[0], -tw_ref[1])
        plane = left_table(row, jnp.concatenate([real, imag], 0))
        @pl.when(me != 0)
        def _():
            for c in range(2):
                for t in range(QUAD):
                    back_send[f, pl.ds(c * QUAD + t, L, stride=8), :] = plane[tile(c), tile(t)]
            spread(back_send.at[f], back_recv.at[f], 8, 3 + f, SHIFTS)

        @pl.when(me == 0)
        def _():
            for c in range(2):
                for t in range(QUAD):
                    zero_send[f, c, pl.ds(t, L, stride=QUAD), :] = plane[tile(c), tile(t)]
                back_recv[c, pl.ds(f * QUAD, QUAD), :] = zero_send[f, c, pl.ds(0, QUAD), :]

            def send_to(shift):
                other, device = shifted(here, *shift)
                for c in range(2):
                    pltpu.make_async_remote_copy(
                        src_ref=zero_send.at[f, c, piece(other, QUAD)],
                        dst_ref=back_recv.at[c, pl.ds(f * QUAD, QUAD)],
                        send_sem=send_sems.at[3 + c],
                        recv_sem=recv_sems.at[3 + c],
                        device_id=device,
                        device_id_type=MESH,
                    ).start()

            @pl.loop(0, 16)
            def _(step):
                dx, dy = step & 3, step >> 2
                pl.when(step != 0)(lambda: send_to((0, dy, dx, 0)))
                for n in range(1, 8):
                    dz, dc = n >> 1, n & 1
                    send_to((dz, dy + n, dx + dz, dc))

    for index in range(7, 10):
        fetches[index].wait()
    zb = (zb_ref[0], zb_ref[1])

    def fold(start, rows):
        for h in range(2):
            half_y[h, pl.ds(start, rows.shape[0]), :] = rows[:, tile(h)]

    def pair_rows(start, count):
        rows = [
            half_y[h, pl.ds(start, count, stride=2), :] + half_y[h, pl.ds(start + 1, count, stride=2), :]
            for h in range(2)
        ]
        return jnp.concatenate(rows, 1)

    def z_pool(values, lanes):
        high, low = parts(values)
        pool = pool_ref[:, lanes]
        return product(high, pool, ((1,), (0,))) + product(low, pool, ((1,), (0,)))

    def across(send, recv, slot):
        own = pltpu.make_async_copy(send.at[my_py], recv.at[my_py], local_sems.at[slot])
        own.start()
        for dx, low in LINE:
            other = (((my_py >> 2) + dx) & 3) * 4 + ((my_py & 3) ^ low)
            pltpu.make_async_remote_copy(
                src_ref=send.at[other],
                dst_ref=recv.at[my_py],
                send_sem=send_sems.at[slot],
                recv_sem=recv_sems.at[slot],
                device_id={"py": other},
                device_id_type=MESH,
            ).start()
        rest = pl.ds(0, PY - 1)
        whole = pltpu.make_async_remote_copy(
            src_ref=send.at[rest],
            dst_ref=recv.at[rest],
            send_sem=send_sems.at[slot],
            recv_sem=recv_sems.at[slot],
            device_id={"py": my_py ^ 1},
            device_id_type=MESH,
        )
        return [own, whole]

    def coarse(f):
        tiles = [
            [back_recv[f, pl.ds(c * QUAD + t, L, stride=8), :] for t in range(QUAD)]
            for c in range(2)
        ]
        waves = jnp.concatenate([jnp.concatenate(part, 1) for part in tiles], 0)
        cells = right_table(waves, zb, ((0,), (0,)))
        cells = jnp.exp(0.5 * cells)
        start = f * 4 * CY * 2
        for t in range(QUAD):
            xs, ys = quarter(t)
            block = cells[tile(t)].reshape(8, 16, LZ)
            mod_ref[f, xs, ys, :] = block
            half_x = block.reshape(4, 2, 16, LZ)
            half_x = half_x[:, 0] + half_x[:, 1]
            for x in range(4):
                fold(start + ((t // 2) * 4 + x) * CY + (t % 2) * 16, half_x[x])
        stored = pltpu.make_async_copy(mod_ref.at[f], mod_out.at[f], fetch_sems.at[len(fetches) + f])
        stored.start()
        rows_one = pair_rows(start, 8 * 16)
        one = z_pool(rows_one, slice(0, 128))
        for i in range(PY):
            one_send[f, i] = one[i * 8 : i * 8 + 8]
        return stored, rows_one, across(one_send.at[f], (one_recv_0, one_recv_1)[f], 7 + f)

    def choose(source, target, pieces):
        for g in range(PY):
            for level, rows in pieces:
                target[g, rows, :] = source[group_ref[level, g], rows, :]

    landed(back_send.at[0], back_recv.at[0], 8, 3, True)
    stored_0, rows_0, one_0 = coarse(0)
    landed(back_send.at[1], back_recv.at[1], 8, 4, True)
    stored_1, rows_1, one_1 = coarse(1)
    rows_one = jnp.concatenate([rows_0, rows_1], 0)
    pairs = rows_one.reshape(2 * 4, 2, 16, LZ)
    fold(0, (pairs[:, 0] + pairs[:, 1]).reshape(2 * 4 * 16, LZ))
    rows_two = pair_rows(0, 2 * 4 * 8)
    pairs = rows_two.reshape(2 * 2, 2, 8, LZ)
    fold(0, (pairs[:, 0] + pairs[:, 1]).reshape(2 * 2 * 8, LZ))
    rows_three = pair_rows(0, 2 * 2 * 4)
    rest = z_pool(jnp.concatenate([rows_two, rows_three], 0), slice(128, 256))
    for i in range(PY):
        rest_send[i, pl.ds(0, 4), :] = rest[i * 4 : i * 4 + 4]
        rest_send[i, pl.ds(4, 1), :] = rest[64 + i : 65 + i]
        rest_send[i, pl.ds(5, 3), :] = jnp.zeros((3, L), F32)
        rest_back[i, pl.ds(5, 3), :] = jnp.zeros((3, L), F32)
    rest_0 = across(rest_send, rest_recv, 9)
    for copy in one_0:
        copy.wait()
    choose(one_recv_0, one_back.at[0], [(0, pl.ds(0, 8))])
    last = across(one_back.at[0], one_out.at[0], 10)
    for copy in one_1:
        copy.wait()
    choose(one_recv_1, one_back.at[1], [(0, pl.ds(0, 8))])
    last += across(one_back.at[1], one_out.at[1], 11)
    for copy in rest_0:
        copy.wait()
    choose(rest_recv, rest_back, [(1, pl.ds(0, 4)), (2, pl.ds(4, 1))])
    last += across(rest_back, rest_out, 12)
    for copy in last:
        copy.wait()
    stored_0.wait()
    stored_1.wait()


def store_kernel(
    mod_in, one_in, rest_in, mod_out, one_out, two_out, three_out,
    mod_ref, one_held, rest_held, one_ref, two_ref, three_ref, in_sems, out_sems,
):
    pairs = [(mod_in.at[f, pl.ds(h * 8, 8)], mod_ref.at[f, pl.ds(h * 8, 8)]) for f in range(2) for h in range(2)]
    pairs += [(one_in, one_held), (rest_in, rest_held)]
    outs = [(mod_ref.at[f, pl.ds(h * 8, 8)], mod_out.at[f, pl.ds(h * 8, 8)]) for f in range(2) for h in range(2)]
    outs += [(one_ref, one_out), (two_ref, two_out), (three_ref, three_out)]
    loads = [pltpu.make_async_copy(*pair, in_sems.at[i]) for i, pair in enumerate(pairs)]
    stores = [pltpu.make_async_copy(*pair, out_sems.at[i]) for i, pair in enumerate(outs)]
    for load in loads[4:] + loads[:4]:
        load.start()
    loads[4].wait()
    loads[5].wait()
    for f in range(2):
        one_ref[f] = one_held[f].reshape(8, 16, L)
        for x in range(4):
            for h in range(2):
                two_ref[f, x, pl.ds(h * 4, 4), :] = rest_held[(f * 4 + x) * 2 + h, pl.ds(0, 4), :][:, :64]
        for x in range(2):
            for y in range(4):
                row = rest_held[(f * 2 + x) * 4 + y, pl.ds(4, 1), :]
                three_ref[f, x, pl.ds(y, 1), :] = row[:, 64:96]
    for store in stores[4:]:
        store.start()
    for i in range(4):
        loads[i].wait()
        stores[i].start()
    for store in stores:
        store.wait()


def on_device(white_noise, spectrum, group_table):
    shapes = [
        white_noise.shape,
        (2, CX // 2, CY // 2, LZ // 2),
        (2, CX // 4, CY // 4, LZ // 4),
        (2, CX // 8, CY // 8, LZ // 8),
    ]
    hbm = pl.BlockSpec(memory_space=pltpu.HBM)
    wide = pltpu.VMEM((2, DEV * 8, L), F32)
    thin = pltpu.VMEM((DEV * QUAD, L), F32)
    table = pltpu.VMEM((QUAD, L, L), F32)
    one, rest = (2, PY, 8, L), (PY, 8, L)
    slots = 13
    operands = [white_noise, spectrum] + tables()
    results = pl.pallas_call(
        kernel,
        out_shape=[jax.ShapeDtypeStruct(shape, F32) for shape in (shapes[0], one, rest)],
        in_specs=[hbm] * (len(operands) + 1),
        out_specs=[hbm] * 3,
        scratch_shapes=[pltpu.SMEM(group_table.shape, jnp.int32)]
        + [pltpu.VMEM(value.shape, value.dtype) for value in operands]
        + [thin, thin, pltpu.VMEM((QUAD, L), F32)]
        + [pltpu.VMEM((size, QUAD, L), F32) for size in (PY, DEV)]
        + [table, table, wide, wide, wide, wide, pltpu.VMEM((2, 2, DEV * QUAD, L), F32)]
        + [pltpu.VMEM(shapes[0], F32), pltpu.VMEM((2, 2 * 8 * CY, L), F32)]
        + [pltpu.VMEM(shape, F32) for shape in (one, rest, rest, one, rest, rest, rest)]
        + [pltpu.SemaphoreType.DMA((size,)) for size in (len(operands) + 3, slots, slots, slots)],
        compiler_params=pltpu.CompilerParams(
            collective_id=0, has_side_effects=True, vmem_limit_bytes=67_043_328
        ),
    )(group_table, *operands)
    return pl.pallas_call(
        store_kernel,
        out_shape=[jax.ShapeDtypeStruct(shape, F32) for shape in shapes],
        in_specs=[hbm] * 3,
        out_specs=[hbm] * 4,
        scratch_shapes=[pltpu.VMEM(shape, F32) for shape in (shapes[0], one, rest, *shapes[1:])]
        + [pltpu.SemaphoreType.DMA((8,)), pltpu.SemaphoreType.DMA((8,))],
        compiler_params=pltpu.CompilerParams(vmem_limit_bytes=67_043_328),
    )(*results)


def solution(mesh):
    in_specs = (P(None, "px", "py", None), P("px", "py", None), P())
    out_specs = (P(None, "px", "py", None),) * 4
    return jax.shard_map(
        on_device, mesh=mesh, in_specs=in_specs, out_specs=out_specs, check_vma=False
    )
```

```python
import numpy as np

import jax
import jax.numpy as jnp
from jax import lax
from jax.experimental import pallas as pl
from jax.experimental.pallas import tpu as pltpu
from jax.sharding import PartitionSpec as P

MESH = pl.DeviceIdType.MESH
F32, BF16 = jnp.float32, jnp.bfloat16
PX, PY = 8, 16
DEV = PX * PY
LX, LY, LZ = 128, 512, 256
CX, CY = LX // PX, LY // PY
L = 128
QUAD = 4


def split(values):
    values = np.asarray(values, np.float32)
    high = values.astype(jnp.bfloat16)
    low = (values - high.astype(np.float32)).astype(jnp.bfloat16)
    return np.stack([high, low], 0)


def tables():
    k = np.arange(L)
    z = np.arange(LZ)
    angle = 2.0 * np.pi / LZ * (k[:, None] * z[None, :] % LZ)
    nyquist = np.where(z % 2 == 0, 1.0, -1.0)
    ahead = np.stack([np.cos(angle), -np.sin(angle)], 0)
    back = 2.0 * ahead
    ahead[1, 0] = nyquist
    back[0, 0] = 1.0
    back[1, 0] = nyquist
    z_ahead = split(ahead.reshape(LZ, LZ))
    z_back = split(back.reshape(LZ, LZ) / (LX * LY * LZ))
    first, second = k // 16, k % 16
    turn = first[:, None] * first[None, :] / 8.0 + second[:, None] * second[None, :] / 16.0
    cos, sin = np.cos(2 * np.pi * turn), -np.sin(2 * np.pi * turn)
    column = split(np.block([[cos, -sin], [sin, cos]]))
    row = split(np.block([[cos, sin], [-sin, cos]]))
    twiddle, small = [], []
    for t in range(QUAD):
        xl = (t // 2) * 8 + first
        yl = (t % 2) * 16 + second
        turn = first[:, None] * xl[None, :] / LX + second[:, None] * yl[None, :] / LY
        twiddle.append(np.stack([np.cos(2 * np.pi * turn), -np.sin(2 * np.pi * turn)], 0))
        turn = (t // 2) * first / 16.0 + (t % 2) * second / 32.0
        small.append(np.stack([np.cos(2 * np.pi * turn), -np.sin(2 * np.pi * turn)], 0))
    twiddle = np.concatenate(twiddle, 2).astype(np.float32)
    small = np.stack(small, 1).reshape(2 * QUAD, L).astype(np.float32)
    pool = np.zeros((LZ, LZ))
    pool[z, z // 2] = 1.0 / 8
    pool[z, 128 + z // 4] = 1.0 / 64
    pool[z, 192 + z // 8] = 1.0 / 512
    return [
        jnp.asarray(v)
        for v in (z_ahead, z_back, column, row, twiddle, small, pool.astype(jnp.bfloat16))
    ]


def parts(values):
    high = values.astype(BF16)
    return high, (values - high.astype(F32)).astype(BF16)


def product(left, right, dims):
    return lax.dot_general(left, right, (dims, ((), ())), preferred_element_type=F32)


def left_table(table, values, dims=((1,), (0,))):
    high, low = parts(values)
    first = product(table[0], high, dims) + product(table[0], low, dims)
    return first + product(table[1], high, dims)


def right_table(values, table, dims=((1,), (0,))):
    high, low = parts(values)
    first = product(high, table[0], dims) + product(low, table[0], dims)
    return first + product(high, table[1], dims)


def hops(shift):
    return sum(min(d, 4 - d) for d in shift[:3])


SHIFTS = [(dz, dy, dx, dc) for dz in range(4) for dy in range(4) for dx in range(4) for dc in range(2)]


def spread_evenly(shifts):
    load = np.zeros(6)
    order, left = [], list(shifts)
    while left:
        def cost(shift):
            after = load.copy()
            for axis, d in enumerate(shift[:3]):
                after[2 * axis] += (0, 1, 1, 0)[d]
                after[2 * axis + 1] += (0, 0, 1, 1)[d]
            return after.max() - after.min()
        best = min(left, key=cost)
        for axis, d in enumerate(best[:3]):
            load[2 * axis] += (0, 1, 1, 0)[d]
            load[2 * axis + 1] += (0, 0, 1, 1)[d]
        left.remove(best)
        order.append(best)
    return order


MIXED = spread_evenly([SHIFTS[(i * 37) % 128] for i in range(1, 128)])
SHIFTS = sorted(SHIFTS[1:], key=lambda shift: -hops(shift))

LINE = [(dx, low) for dx in range(4) for low in range(4)]
LINE = sorted(LINE[1:], key=lambda move: -min(move[0], 4 - move[0]) - (move[1] >> 1))


def place():
    px, py = lax.axis_index("px"), lax.axis_index("py")
    return (px >> 2) * 2 + ((py >> 1) & 1), px & 3, py >> 2, py & 1


def shifted(here, dz, dy, dx, dc):
    z, y, x = ((here[i] + d) & 3 for i, d in enumerate((dz, dy, dx)))
    px = (z >> 1) * 4 + y
    py = x * 4 + (z & 1) * 2 + (here[3] ^ dc)
    return px * PY + py, {"px": px, "py": py}


def quarter(t):
    return slice((t // 2) * 8, (t // 2) * 8 + 8), slice((t % 2) * 16, (t % 2) * 16 + 16)


def tile(t):
    return slice(t * L, (t + 1) * L)


def butterfly(values):
    a, b, c, d = values
    p, q, r, s = a + b, a - b, c + d, c - d
    return [p + r, q + s, p - r, q - s]


def turned(real, imag, cos, sin):
    return real * cos - imag * sin, real * sin + imag * cos


def piece(index, height):
    return pl.ds(pl.multiple_of(index * height, height), height)


def kernel(
    group_in, noise_in, spec_in, za_in, zb_in, col_in, row_in, tw_in, small_in, pool_in,
    mod_out, one_out, rest_out,
    group_ref, noise_ref, spec_ref, za_ref, zb_ref, col_ref, row_ref, tw_ref, small_ref, pool_ref,
    s_send, s_recv, n_send, n_line, n_recv, u_table, v_table, ahead_send, ahead_recv, back_send, back_recv, zero_send,
    half_y, one_send, one_recv_0, one_recv_1, one_back, rest_send, rest_recv, rest_back,
    fetch_sems, local_sems, send_sems, recv_sems,
):
    here = place()
    my_px, my_py = lax.axis_index("px"), lax.axis_index("py")
    me = my_px * PY + my_py
    barrier = pltpu.get_barrier_semaphore()

    pairs = (
        (spec_in, spec_ref), (noise_in, noise_ref), (za_in, za_ref), (col_in, col_ref),
        (row_in, row_ref), (tw_in, tw_ref), (small_in, small_ref), (zb_in, zb_ref),
        (pool_in, pool_ref), (group_in, group_ref),
    )
    fetches = [
        pltpu.make_async_copy(source, target, fetch_sems.at[index])
        for index, (source, target) in enumerate(pairs)
    ]
    for fetch in fetches:
        fetch.start()

    for shift in SHIFTS:
        pl.semaphore_signal(barrier, inc=1, device_id=shifted(here, *shift)[1], device_id_type=MESH)

    def spread(send, recv, height, slot, order=MIXED):
        pltpu.make_async_copy(
            send.at[piece(me, height)], recv.at[piece(me, height)], local_sems.at[slot]
        ).start()

        def send_to(shift):
            other, device = shifted(here, *shift)
            pltpu.make_async_remote_copy(
                src_ref=send.at[piece(other, height)],
                dst_ref=recv.at[piece(me, height)],
                send_sem=send_sems.at[slot],
                recv_sem=recv_sems.at[slot],
                device_id=device,
                device_id_type=MESH,
            ).start()

        for shift in order:
            send_to(shift)

    def landed(send, recv, height, slot, packed=False):
        own = pltpu.make_async_copy(
            send.at[piece(me, height)], recv.at[piece(me, height)], local_sems.at[slot]
        )
        if packed:
            pl.when(me != 0)(own.wait)
        else:
            own.wait()
        rest = pl.ds(0, (DEV - 1) * height)
        whole = pltpu.make_async_remote_copy(
            src_ref=send.at[rest],
            dst_ref=recv.at[rest],
            send_sem=send_sems.at[slot],
            recv_sem=recv_sems.at[slot],
            device_id=shifted(here, 0, 0, 0, 1)[1],
            device_id_type=MESH,
        )
        whole.wait()

    fetches[0].wait()
    for t in range(QUAD):
        xs, ys = quarter(t)
        block = spec_ref[xs, ys, :].reshape(L, LZ)
        s_send[pl.ds(t, L, stride=QUAD), :] = block[:, :L].T
        n_send[pl.ds(t, 1), :] = block[:, L:].T[:1]

    fetches[1].wait()
    fetches[2].wait()
    za = (za_ref[0], za_ref[1])

    def z_ahead(f):
        rows = [noise_ref[(f,) + quarter(t)].reshape(L, LZ) for t in range(QUAD)]
        return left_table(za, jnp.concatenate(rows, 0), ((1,), (1,)))

    values = [z_ahead(0), z_ahead(1)]
    at_zero = lax.broadcasted_iota(jnp.int32, (L, QUAD * L), 0) == 0
    real_one = jnp.where(at_zero, values[0][L:], values[1][:L])
    imag_zero = jnp.where(at_zero, values[1][:L], values[0][L:])
    members = ((values[0][:L], imag_zero), (real_one, values[1][L:]))
    for f in range(2):
        for c in range(2):
            for t in range(QUAD):
                ahead_send[f, pl.ds(c * QUAD + t, L, stride=8), :] = members[f][c][:, tile(t)]

    pl.semaphore_wait(barrier, DEV - 1)
    line_copy = pltpu.make_async_remote_copy(
        src_ref=n_send,
        dst_ref=n_line.at[my_py],
        send_sem=send_sems.at[5],
        recv_sem=recv_sems.at[5],
        device_id={"py": 0},
        device_id_type=MESH,
    )
    plane_copies = [
        pltpu.make_async_remote_copy(
            src_ref=n_line.at[i],
            dst_ref=n_recv.at[my_px * PY + i],
            send_sem=send_sems.at[6],
            recv_sem=recv_sems.at[6],
            device_id={"px": 0},
            device_id_type=MESH,
        )
        for i in range(PY)
    ]

    def line_rest(device):
        rest = n_line.at[pl.ds(1, PY - 1)]
        return pltpu.make_async_remote_copy(
            src_ref=rest, dst_ref=rest, send_sem=send_sems.at[5], recv_sem=recv_sems.at[5],
            device_id=device, device_id_type=MESH,
        )

    def plane_rest(rest, device):
        return pltpu.make_async_remote_copy(
            src_ref=rest, dst_ref=rest, send_sem=send_sems.at[6], recv_sem=recv_sems.at[6],
            device_id=device, device_id_type=MESH,
        )

    pl.when(my_py != 0)(line_copy.start)
    spread(s_send, s_recv, QUAD, 0)

    spread(ahead_send.at[0], ahead_recv.at[0], 8, 1)

    @pl.when(my_py == 0)
    def _():
        n_line[0] = n_send[...]
        line_rest({"py": 1}).wait_recv()

        @pl.when(my_px != 0)
        def _():
            for copy in plane_copies:
                copy.start()

    spread(ahead_send.at[1], ahead_recv.at[1], 8, 2, SHIFTS)

    landed(s_send, s_recv, QUAD, 0)
    for t in range(QUAD):
        u_table[t] = s_recv[pl.ds(t, L, stride=QUAD), :].T

    pl.when(my_py != 0)(line_copy.wait_send)
    for index in range(3, 7):
        fetches[index].wait()

    def last_table():
        @pl.when(me != 0)
        def _():
            v_table[...] = u_table[...]

        @pl.when((my_py == 0) & (my_px != 0))
        def _():
            plane_rest(n_line, {"px": 0}).wait_send()

        @pl.when(me == 0)
        def _():
            n_recv[pl.ds(0, PY)] = n_line[...]
            plane_rest(n_recv.at[pl.ds(PY, DEV - PY)], {"px": 1}).wait_recv()
            for t in range(QUAD):
                v_table[t] = n_recv[:, t, :].T

    column = (col_ref[0], col_ref[1])
    row = (row_ref[0], row_ref[1])
    for f in range(2):
        landed(ahead_send.at[f], ahead_recv.at[f], 8, 1 + f)
        if f == 1:
            last_table()
        plane = [
            jnp.concatenate(
                [ahead_recv[f, pl.ds(c * QUAD + t, L, stride=8), :] for t in range(QUAD)], 1
            )
            for c in range(2)
        ]
        mixed = left_table(column, jnp.concatenate(plane, 0))
        real, imag = turned(mixed[:L], mixed[L:], tw_ref[0], tw_ref[1])
        reals = butterfly([real[:, tile(t)] for t in range(QUAD)])
        imags = butterfly([imag[:, tile(t)] for t in range(QUAD)])
        rows = []
        for t in range(QUAD):
            cos, sin = small_ref[pl.ds(t, 1), :], small_ref[pl.ds(QUAD + t, 1), :]
            pair = turned(reals[t], imags[t], cos, sin) if t else (reals[t], imags[t])
            rows.append(jnp.concatenate(pair, 1))
        freq = right_table(jnp.concatenate(rows, 0), row)
        table = u_table if f == 0 else v_table
        scale = jnp.concatenate([table[t] for t in range(QUAD)], 0)
        freq = freq * jnp.concatenate([scale, scale], 1)
        mixed = right_table(freq, column)
        reals, imags = [], []
        for t in range(QUAD):
            part = mixed[tile(t)]
            pair = (part[:, :L], part[:, L:])
            if t:
                cos, sin = small_ref[pl.ds(t, 1), :], small_ref[pl.ds(QUAD + t, 1), :]
                pair = turned(*pair, cos, -sin)
            reals.append(pair[0])
            imags.append(pair[1])
        real = jnp.concatenate(butterfly(reals), 1)
        imag = jnp.concatenate(butterfly(imags), 1)
        real, imag = turned(real, imag, tw_ref[0], -tw_ref[1])
        plane = left_table(row, jnp.concatenate([real, imag], 0))
        @pl.when(me != 0)
        def _():
            for c in range(2):
                for t in range(QUAD):
                    back_send[f, pl.ds(c * QUAD + t, L, stride=8), :] = plane[tile(c), tile(t)]
            spread(back_send.at[f], back_recv.at[f], 8, 3 + f, SHIFTS)

        @pl.when(me == 0)
        def _():
            for c in range(2):
                for t in range(QUAD):
                    zero_send[f, c, pl.ds(t, L, stride=QUAD), :] = plane[tile(c), tile(t)]
                back_recv[c, pl.ds(f * QUAD, QUAD), :] = zero_send[f, c, pl.ds(0, QUAD), :]

            def send_to(shift):
                other, device = shifted(here, *shift)
                for c in range(2):
                    pltpu.make_async_remote_copy(
                        src_ref=zero_send.at[f, c, piece(other, QUAD)],
                        dst_ref=back_recv.at[c, pl.ds(f * QUAD, QUAD)],
                        send_sem=send_sems.at[3 + c],
                        recv_sem=recv_sems.at[3 + c],
                        device_id=device,
                        device_id_type=MESH,
                    ).start()

            @pl.loop(0, 16)
            def _(step):
                dx, dy = step & 3, step >> 2
                pl.when(step != 0)(lambda: send_to((0, dy, dx, 0)))
                for n in range(1, 8):
                    dz, dc = n >> 1, n & 1
                    send_to((dz, dy + n, dx + dz, dc))

    for index in range(7, 10):
        fetches[index].wait()
    zb = (zb_ref[0], zb_ref[1])

    def fold(start, rows):
        for h in range(2):
            half_y[h, pl.ds(start, rows.shape[0]), :] = rows[:, tile(h)]

    def pair_rows(start, count):
        rows = [
            half_y[h, pl.ds(start, count, stride=2), :] + half_y[h, pl.ds(start + 1, count, stride=2), :]
            for h in range(2)
        ]
        return jnp.concatenate(rows, 1)

    def z_pool(values, lanes):
        high, low = parts(values)
        pool = pool_ref[:, lanes]
        return product(high, pool, ((1,), (0,))) + product(low, pool, ((1,), (0,)))

    def across(send, recv, slot):
        own = pltpu.make_async_copy(send.at[my_py], recv.at[my_py], local_sems.at[slot])
        own.start()
        for dx, low in LINE:
            other = (((my_py >> 2) + dx) & 3) * 4 + ((my_py & 3) ^ low)
            pltpu.make_async_remote_copy(
                src_ref=send.at[other],
                dst_ref=recv.at[my_py],
                send_sem=send_sems.at[slot],
                recv_sem=recv_sems.at[slot],
                device_id={"py": other},
                device_id_type=MESH,
            ).start()
        rest = pl.ds(0, PY - 1)
        whole = pltpu.make_async_remote_copy(
            src_ref=send.at[rest],
            dst_ref=recv.at[rest],
            send_sem=send_sems.at[slot],
            recv_sem=recv_sems.at[slot],
            device_id={"py": my_py ^ 1},
            device_id_type=MESH,
        )
        return [own, whole]

    def coarse(f):
        tiles = [
            [back_recv[f, pl.ds(c * QUAD + t, L, stride=8), :] for t in range(QUAD)]
            for c in range(2)
        ]
        waves = jnp.concatenate([jnp.concatenate(part, 1) for part in tiles], 0)
        cells = right_table(waves, zb, ((0,), (0,)))
        cells = jnp.exp(0.5 * cells)
        start = f * 4 * CY * 2
        for t in range(QUAD):
            xs, ys = quarter(t)
            block = cells[tile(t)].reshape(8, 16, LZ)
            mod_out[f, xs, ys, :] = block
            half_x = block.reshape(4, 2, 16, LZ)
            half_x = half_x[:, 0] + half_x[:, 1]
            for x in range(4):
                fold(start + ((t // 2) * 4 + x) * CY + (t % 2) * 16, half_x[x])
        rows_one = pair_rows(start, 8 * 16)
        one = z_pool(rows_one, slice(0, 128))
        for i in range(PY):
            one_send[f, i] = one[i * 8 : i * 8 + 8]
        return rows_one, across(one_send.at[f], (one_recv_0, one_recv_1)[f], 7 + f)

    def choose(source, target, pieces):
        for g in range(PY):
            for level, rows in pieces:
                target[g, rows, :] = source[group_ref[level, g], rows, :]

    landed(back_send.at[0], back_recv.at[0], 8, 3, True)
    rows_0, one_0 = coarse(0)
    landed(back_send.at[1], back_recv.at[1], 8, 4, True)
    rows_1, one_1 = coarse(1)
    rows_one = jnp.concatenate([rows_0, rows_1], 0)
    pairs = rows_one.reshape(2 * 4, 2, 16, LZ)
    fold(0, (pairs[:, 0] + pairs[:, 1]).reshape(2 * 4 * 16, LZ))
    rows_two = pair_rows(0, 2 * 4 * 8)
    pairs = rows_two.reshape(2 * 2, 2, 8, LZ)
    fold(0, (pairs[:, 0] + pairs[:, 1]).reshape(2 * 2 * 8, LZ))
    rows_three = pair_rows(0, 2 * 2 * 4)
    rest = z_pool(jnp.concatenate([rows_two, rows_three], 0), slice(128, 256))
    for i in range(PY):
        rest_send[i, pl.ds(0, 4), :] = rest[i * 4 : i * 4 + 4]
        rest_send[i, pl.ds(4, 1), :] = rest[64 + i : 65 + i]
        rest_send[i, pl.ds(5, 3), :] = jnp.zeros((3, L), F32)
        rest_back[i, pl.ds(5, 3), :] = jnp.zeros((3, L), F32)
    rest_0 = across(rest_send, rest_recv, 9)
    for copy in one_0:
        copy.wait()
    choose(one_recv_0, one_back.at[0], [(0, pl.ds(0, 8))])
    last = across(one_back.at[0], one_out.at[0], 10)
    for copy in one_1:
        copy.wait()
    choose(one_recv_1, one_back.at[1], [(0, pl.ds(0, 8))])
    last += across(one_back.at[1], one_out.at[1], 11)
    for copy in rest_0:
        copy.wait()
    choose(rest_recv, rest_back, [(1, pl.ds(0, 4)), (2, pl.ds(4, 1))])
    last += across(rest_back, rest_out, 12)
    for copy in last:
        copy.wait()


def store_kernel(
    mod_in, one_in, rest_in, mod_out, one_out, two_out, three_out, one_ref, two_ref, three_ref, sems,
):
    outs = [(mod_in, mod_out), (one_ref, one_out), (two_ref, two_out), (three_ref, three_out)]
    stores = [pltpu.make_async_copy(*pair, sems.at[i]) for i, pair in enumerate(outs)]
    stores[0].start()
    for f in range(2):
        one_ref[f] = one_in[f].reshape(8, 16, L)
        for x in range(4):
            for h in range(2):
                two_ref[f, x, pl.ds(h * 4, 4), :] = rest_in[(f * 4 + x) * 2 + h, pl.ds(0, 4), :][:, :64]
        for x in range(2):
            for y in range(4):
                row = rest_in[(f * 2 + x) * 4 + y, pl.ds(4, 1), :]
                three_ref[f, x, pl.ds(y, 1), :] = row[:, 64:96]
    for store in stores[1:]:
        store.start()
    for store in stores:
        store.wait()


def on_device(white_noise, spectrum, group_table):
    shapes = [
        white_noise.shape,
        (2, CX // 2, CY // 2, LZ // 2),
        (2, CX // 4, CY // 4, LZ // 4),
        (2, CX // 8, CY // 8, LZ // 8),
    ]
    hbm = pl.BlockSpec(memory_space=pltpu.HBM)
    wide = pltpu.VMEM((2, DEV * 8, L), F32)
    thin = pltpu.VMEM((DEV * QUAD, L), F32)
    table = pltpu.VMEM((QUAD, L, L), F32)
    one, rest = (2, PY, 8, L), (PY, 8, L)
    slots = 13
    operands = [white_noise, spectrum] + tables()
    results = pl.pallas_call(
        kernel,
        out_shape=[jax.ShapeDtypeStruct(shape, F32) for shape in (shapes[0], one, rest)],
        in_specs=[hbm] * (len(operands) + 1),
        out_specs=[pl.BlockSpec(memory_space=pltpu.VMEM)] * 3,
        scratch_shapes=[pltpu.SMEM(group_table.shape, jnp.int32)]
        + [pltpu.VMEM(value.shape, value.dtype) for value in operands]
        + [thin, thin, pltpu.VMEM((QUAD, L), F32)]
        + [pltpu.VMEM((size, QUAD, L), F32) for size in (PY, DEV)]
        + [table, table, wide, wide, wide, wide, pltpu.VMEM((2, 2, DEV * QUAD, L), F32)]
        + [pltpu.VMEM((2, 2 * 8 * CY, L), F32)]
        + [pltpu.VMEM(shape, F32) for shape in (one, rest, rest, one, rest, rest, rest)]
        + [pltpu.SemaphoreType.DMA((size,)) for size in (len(operands) + 3, slots, slots, slots)],
        compiler_params=pltpu.CompilerParams(
            collective_id=0, has_side_effects=True, vmem_limit_bytes=48 * 1024 * 1024
        ),
    )(*[pltpu.with_memory_space_constraint(v, pltpu.HBM) for v in [group_table] + operands])
    return pl.pallas_call(
        store_kernel,
        out_shape=[jax.ShapeDtypeStruct(shape, F32) for shape in shapes],
        in_specs=[pl.BlockSpec(memory_space=pltpu.VMEM)] * 3,
        out_specs=[hbm] * 4,
        scratch_shapes=[pltpu.VMEM(shape, F32) for shape in shapes[1:]] + [pltpu.SemaphoreType.DMA((4,))],
        compiler_params=pltpu.CompilerParams(vmem_limit_bytes=2 * 1024 * 1024),
    )(*results)


def solution(mesh):
    in_specs = (P(None, "px", "py", None), P("px", "py", None), P())
    out_specs = (P(None, "px", "py", None),) * 4
    return jax.shard_map(
        on_device, mesh=mesh, in_specs=in_specs, out_specs=out_specs, check_vma=False
    )
```

```python
import numpy as np

import jax
import jax.numpy as jnp
from jax import lax
from jax.experimental import pallas as pl
from jax.experimental.pallas import tpu as pltpu
from jax.sharding import PartitionSpec as P

MESH = pl.DeviceIdType.MESH
F32, BF16 = jnp.float32, jnp.bfloat16
PX, PY = 8, 16
DEV = PX * PY
LX, LY, LZ = 128, 512, 256
CX, CY = LX // PX, LY // PY
L = 128
QUAD = 4


def split(values):
    values = np.asarray(values, np.float32)
    high = values.astype(jnp.bfloat16)
    low = (values - high.astype(np.float32)).astype(jnp.bfloat16)
    return np.stack([high, low], 0)


def tables():
    k = np.arange(L)
    z = np.arange(LZ)
    angle = 2.0 * np.pi / LZ * (k[:, None] * z[None, :] % LZ)
    nyquist = np.where(z % 2 == 0, 1.0, -1.0)
    ahead = np.stack([np.cos(angle), -np.sin(angle)], 0)
    back = 2.0 * ahead
    ahead[1, 0] = nyquist
    back[0, 0] = 1.0
    back[1, 0] = nyquist
    z_ahead = split(ahead.reshape(LZ, LZ))
    z_back = split(back.reshape(LZ, LZ) / (LX * LY * LZ))
    first, second = k // 16, k % 16
    turn = first[:, None] * first[None, :] / 8.0 + second[:, None] * second[None, :] / 16.0
    cos, sin = np.cos(2 * np.pi * turn), -np.sin(2 * np.pi * turn)
    column = split(np.block([[cos, -sin], [sin, cos]]))
    row = split(np.block([[cos, sin], [-sin, cos]]))
    twiddle, small = [], []
    for t in range(QUAD):
        xl = (t // 2) * 8 + first
        yl = (t % 2) * 16 + second
        turn = first[:, None] * xl[None, :] / LX + second[:, None] * yl[None, :] / LY
        twiddle.append(np.stack([np.cos(2 * np.pi * turn), -np.sin(2 * np.pi * turn)], 0))
        turn = (t // 2) * first / 16.0 + (t % 2) * second / 32.0
        small.append(np.stack([np.cos(2 * np.pi * turn), -np.sin(2 * np.pi * turn)], 0))
    twiddle = np.concatenate(twiddle, 2).astype(np.float32)
    small = np.stack(small, 1).reshape(2 * QUAD, L).astype(np.float32)
    pool = np.zeros((LZ, LZ))
    pool[z, z // 2] = 1.0 / 8
    pool[z, 128 + z // 4] = 1.0 / 64
    pool[z, 192 + z // 8] = 1.0 / 512
    return [
        jnp.asarray(v)
        for v in (z_ahead, z_back, column, row, twiddle, small, pool.astype(jnp.bfloat16))
    ]


def parts(values):
    high = values.astype(BF16)
    return high, (values - high.astype(F32)).astype(BF16)


def product(left, right, dims):
    return lax.dot_general(left, right, (dims, ((), ())), preferred_element_type=F32)


def left_table(table, values, dims=((1,), (0,))):
    high, low = parts(values)
    first = product(table[0], high, dims) + product(table[0], low, dims)
    return first + product(table[1], high, dims)


def right_table(values, table, dims=((1,), (0,))):
    high, low = parts(values)
    first = product(high, table[0], dims) + product(low, table[0], dims)
    return first + product(high, table[1], dims)


def hops(shift):
    return sum(min(d, 4 - d) for d in shift[:3])


SHIFTS = [(dz, dy, dx, dc) for dz in range(4) for dy in range(4) for dx in range(4) for dc in range(2)]


def spread_evenly(shifts):
    load = np.zeros(6)
    order, left = [], list(shifts)
    while left:
        def cost(shift):
            after = load.copy()
            for axis, d in enumerate(shift[:3]):
                after[2 * axis] += (0, 1, 1, 0)[d]
                after[2 * axis + 1] += (0, 0, 1, 1)[d]
            return after.max() - after.min()
        best = min(left, key=cost)
        for axis, d in enumerate(best[:3]):
            load[2 * axis] += (0, 1, 1, 0)[d]
            load[2 * axis + 1] += (0, 0, 1, 1)[d]
        left.remove(best)
        order.append(best)
    return order


MIXED = spread_evenly([SHIFTS[(i * 37) % 128] for i in range(1, 128)])
SHIFTS = sorted(SHIFTS[1:], key=lambda shift: -hops(shift))

LINE = [(dx, low) for dx in range(4) for low in range(4)]
LINE = sorted(LINE[1:], key=lambda move: -min(move[0], 4 - move[0]) - (move[1] >> 1))


def place():
    px, py = lax.axis_index("px"), lax.axis_index("py")
    return (px >> 2) * 2 + ((py >> 1) & 1), px & 3, py >> 2, py & 1


def shifted(here, dz, dy, dx, dc):
    z, y, x = ((here[i] + d) & 3 for i, d in enumerate((dz, dy, dx)))
    px = (z >> 1) * 4 + y
    py = x * 4 + (z & 1) * 2 + (here[3] ^ dc)
    return px * PY + py, {"px": px, "py": py}


def quarter(t):
    return slice((t // 2) * 8, (t // 2) * 8 + 8), slice((t % 2) * 16, (t % 2) * 16 + 16)


def tile(t):
    return slice(t * L, (t + 1) * L)


def butterfly(values):
    a, b, c, d = values
    p, q, r, s = a + b, a - b, c + d, c - d
    return [p + r, q + s, p - r, q - s]


def turned(real, imag, cos, sin):
    return real * cos - imag * sin, real * sin + imag * cos


def piece(index, height):
    return pl.ds(pl.multiple_of(index * height, height), height)


def kernel(
    group_in, noise_in, spec_in, za_in, zb_in, col_in, row_in, tw_in, small_in, pool_in,
    mod_out, one_out, rest_out,
    group_ref, noise_ref, spec_ref, za_ref, zb_ref, col_ref, row_ref, tw_ref, small_ref, pool_ref,
    s_send, s_recv, n_send, n_line, n_recv, u_table, v_table, ahead_send, ahead_recv, back_send, back_recv, zero_send,
    half_y, one_send, one_recv_0, one_recv_1, one_back, rest_send, rest_recv, rest_back,
    own_sem, fetch_sems, send_sems, recv_sems,
):
    here = place()
    my_px, my_py = lax.axis_index("px"), lax.axis_index("py")
    me = my_px * PY + my_py
    barrier = pltpu.get_barrier_semaphore()

    pairs = (
        (spec_in, spec_ref), (noise_in, noise_ref), (za_in, za_ref), (col_in, col_ref),
        (row_in, row_ref), (tw_in, tw_ref), (small_in, small_ref), (zb_in, zb_ref),
        (pool_in, pool_ref), (group_in, group_ref),
    )
    fetches = [
        pltpu.make_async_copy(source, target, fetch_sems.at[index])
        for index, (source, target) in enumerate(pairs)
    ]
    for fetch in fetches:
        fetch.start()

    for shift in SHIFTS:
        pl.semaphore_signal(barrier, inc=1, device_id=shifted(here, *shift)[1], device_id_type=MESH)

    def spread(send, recv, height, slot, order=MIXED):
        if height == QUAD:
            pltpu.make_async_copy(send.at[piece(me, height)], recv.at[piece(me, height)], own_sem).start()
        else:
            recv[piece(me, height), :] = send[piece(me, height), :]

        def send_to(shift):
            other, device = shifted(here, *shift)
            pltpu.make_async_remote_copy(
                src_ref=send.at[piece(other, height)],
                dst_ref=recv.at[piece(me, height)],
                send_sem=send_sems.at[slot],
                recv_sem=recv_sems.at[slot],
                device_id=device,
                device_id_type=MESH,
            ).start()

        for shift in order:
            send_to(shift)

    def landed(send, recv, height, slot):
        if height == QUAD:
            pltpu.make_async_copy(send.at[piece(me, height)], recv.at[piece(me, height)], own_sem).wait()
        rest = pl.ds(0, (DEV - 1) * height)
        whole = pltpu.make_async_remote_copy(
            src_ref=send.at[rest],
            dst_ref=recv.at[rest],
            send_sem=send_sems.at[slot],
            recv_sem=recv_sems.at[slot],
            device_id=shifted(here, 0, 0, 0, 1)[1],
            device_id_type=MESH,
        )
        whole.wait()

    fetches[0].wait()
    for t in range(QUAD):
        xs, ys = quarter(t)
        block = spec_ref[xs, ys, :].reshape(L, LZ)
        s_send[pl.ds(t, L, stride=QUAD), :] = block[:, :L].T
        n_send[pl.ds(t, 1), :] = block[:, L:].T[:1]

    fetches[1].wait()
    fetches[2].wait()
    za = (za_ref[0], za_ref[1])

    def z_ahead(f):
        rows = [noise_ref[(f,) + quarter(t)].reshape(L, LZ) for t in range(QUAD)]
        return left_table(za, jnp.concatenate(rows, 0), ((1,), (1,)))

    values = [z_ahead(0), z_ahead(1)]
    at_zero = lax.broadcasted_iota(jnp.int32, (L, QUAD * L), 0) == 0
    real_one = jnp.where(at_zero, values[0][L:], values[1][:L])
    imag_zero = jnp.where(at_zero, values[1][:L], values[0][L:])
    members = ((values[0][:L], imag_zero), (real_one, values[1][L:]))
    for f in range(2):
        for c in range(2):
            for t in range(QUAD):
                ahead_send[f, pl.ds(c * QUAD + t, L, stride=8), :] = members[f][c][:, tile(t)]

    pl.semaphore_wait(barrier, DEV - 1)
    line_copy = pltpu.make_async_remote_copy(
        src_ref=n_send,
        dst_ref=n_line.at[my_py],
        send_sem=send_sems.at[5],
        recv_sem=recv_sems.at[5],
        device_id={"py": 0},
        device_id_type=MESH,
    )
    plane_copies = [
        pltpu.make_async_remote_copy(
            src_ref=n_line.at[i],
            dst_ref=n_recv.at[my_px * PY + i],
            send_sem=send_sems.at[6],
            recv_sem=recv_sems.at[6],
            device_id={"px": 0},
            device_id_type=MESH,
        )
        for i in range(PY)
    ]

    def line_rest(device):
        rest = n_line.at[pl.ds(1, PY - 1)]
        return pltpu.make_async_remote_copy(
            src_ref=rest, dst_ref=rest, send_sem=send_sems.at[5], recv_sem=recv_sems.at[5],
            device_id=device, device_id_type=MESH,
        )

    def plane_rest(rest, device):
        return pltpu.make_async_remote_copy(
            src_ref=rest, dst_ref=rest, send_sem=send_sems.at[6], recv_sem=recv_sems.at[6],
            device_id=device, device_id_type=MESH,
        )

    pl.when(my_py != 0)(line_copy.start)
    spread(s_send, s_recv, QUAD, 0)

    spread(ahead_send.at[0], ahead_recv.at[0], 8, 1)

    @pl.when(my_py == 0)
    def _():
        n_line[0] = n_send[...]
        line_rest({"py": 1}).wait_recv()

        @pl.when(my_px != 0)
        def _():
            for copy in plane_copies:
                copy.start()

    spread(ahead_send.at[1], ahead_recv.at[1], 8, 2, SHIFTS)

    landed(s_send, s_recv, QUAD, 0)
    for t in range(QUAD):
        u_table[t] = s_recv[pl.ds(t, L, stride=QUAD), :].T

    pl.when(my_py != 0)(line_copy.wait_send)
    for index in range(3, 7):
        fetches[index].wait()

    def last_table():
        @pl.when(me != 0)
        def _():
            v_table[...] = u_table[...]

        @pl.when((my_py == 0) & (my_px != 0))
        def _():
            plane_rest(n_line, {"px": 0}).wait_send()

        @pl.when(me == 0)
        def _():
            n_recv[pl.ds(0, PY)] = n_line[...]
            plane_rest(n_recv.at[pl.ds(PY, DEV - PY)], {"px": 1}).wait_recv()
            for t in range(QUAD):
                v_table[t] = n_recv[:, t, :].T

    column = (col_ref[0], col_ref[1])
    row = (row_ref[0], row_ref[1])
    for f in range(2):
        landed(ahead_send.at[f], ahead_recv.at[f], 8, 1 + f)
        if f == 1:
            last_table()
        plane = [
            jnp.concatenate(
                [ahead_recv[f, pl.ds(c * QUAD + t, L, stride=8), :] for t in range(QUAD)], 1
            )
            for c in range(2)
        ]
        mixed = left_table(column, jnp.concatenate(plane, 0))
        real, imag = turned(mixed[:L], mixed[L:], tw_ref[0], tw_ref[1])
        reals = butterfly([real[:, tile(t)] for t in range(QUAD)])
        imags = butterfly([imag[:, tile(t)] for t in range(QUAD)])
        rows = []
        for t in range(QUAD):
            cos, sin = small_ref[pl.ds(t, 1), :], small_ref[pl.ds(QUAD + t, 1), :]
            pair = turned(reals[t], imags[t], cos, sin) if t else (reals[t], imags[t])
            rows.append(jnp.concatenate(pair, 1))
        freq = right_table(jnp.concatenate(rows, 0), row)
        table = u_table if f == 0 else v_table
        scale = jnp.concatenate([table[t] for t in range(QUAD)], 0)
        freq = freq * jnp.concatenate([scale, scale], 1)
        mixed = right_table(freq, column)
        reals, imags = [], []
        for t in range(QUAD):
            part = mixed[tile(t)]
            pair = (part[:, :L], part[:, L:])
            if t:
                cos, sin = small_ref[pl.ds(t, 1), :], small_ref[pl.ds(QUAD + t, 1), :]
                pair = turned(*pair, cos, -sin)
            reals.append(pair[0])
            imags.append(pair[1])
        real = jnp.concatenate(butterfly(reals), 1)
        imag = jnp.concatenate(butterfly(imags), 1)
        real, imag = turned(real, imag, tw_ref[0], -tw_ref[1])
        plane = left_table(row, jnp.concatenate([real, imag], 0))
        @pl.when(me != 0)
        def _():
            for c in range(2):
                for t in range(QUAD):
                    back_send[f, pl.ds(c * QUAD + t, L, stride=8), :] = plane[tile(c), tile(t)]
            spread(back_send.at[f], back_recv.at[f], 8, 3 + f, SHIFTS)

        @pl.when(me == 0)
        def _():
            for c in range(2):
                for t in range(QUAD):
                    zero_send[f, c, pl.ds(t, L, stride=QUAD), :] = plane[tile(c), tile(t)]
                back_recv[c, pl.ds(f * QUAD, QUAD), :] = zero_send[f, c, pl.ds(0, QUAD), :]

            def send_to(shift):
                other, device = shifted(here, *shift)
                for c in range(2):
                    pltpu.make_async_remote_copy(
                        src_ref=zero_send.at[f, c, piece(other, QUAD)],
                        dst_ref=back_recv.at[c, pl.ds(f * QUAD, QUAD)],
                        send_sem=send_sems.at[3 + c],
                        recv_sem=recv_sems.at[3 + c],
                        device_id=device,
                        device_id_type=MESH,
                    ).start()

            @pl.loop(0, 16)
            def _(step):
                dx, dy = step & 3, step >> 2
                pl.when(step != 0)(lambda: send_to((0, dy, dx, 0)))
                for n in range(1, 8):
                    dz, dc = n >> 1, n & 1
                    send_to((dz, dy + n, dx + dz, dc))

    for index in range(7, 10):
        fetches[index].wait()
    zb = (zb_ref[0], zb_ref[1])

    def fold(start, rows):
        for h in range(2):
            half_y[h, pl.ds(start, rows.shape[0]), :] = rows[:, tile(h)]

    def pair_rows(start, count):
        rows = [
            half_y[h, pl.ds(start, count, stride=2), :] + half_y[h, pl.ds(start + 1, count, stride=2), :]
            for h in range(2)
        ]
        return jnp.concatenate(rows, 1)

    def z_pool(values, lanes):
        high, low = parts(values)
        pool = pool_ref[:, lanes]
        return product(high, pool, ((1,), (0,))) + product(low, pool, ((1,), (0,)))

    def across(send, recv, slot):
        recv[my_py] = send[my_py]
        for dx, low in LINE:
            other = (((my_py >> 2) + dx) & 3) * 4 + ((my_py & 3) ^ low)
            pltpu.make_async_remote_copy(
                src_ref=send.at[other],
                dst_ref=recv.at[my_py],
                send_sem=send_sems.at[slot],
                recv_sem=recv_sems.at[slot],
                device_id={"py": other},
                device_id_type=MESH,
            ).start()
        rest = pl.ds(0, PY - 1)
        whole = pltpu.make_async_remote_copy(
            src_ref=send.at[rest],
            dst_ref=recv.at[rest],
            send_sem=send_sems.at[slot],
            recv_sem=recv_sems.at[slot],
            device_id={"py": my_py ^ 1},
            device_id_type=MESH,
        )
        return whole

    def coarse(f):
        tiles = [
            [back_recv[f, pl.ds(c * QUAD + t, L, stride=8), :] for t in range(QUAD)]
            for c in range(2)
        ]
        waves = jnp.concatenate([jnp.concatenate(part, 1) for part in tiles], 0)
        cells = right_table(waves, zb, ((0,), (0,)))
        cells = jnp.exp(0.5 * cells)
        start = f * 4 * CY * 2
        for t in range(QUAD):
            xs, ys = quarter(t)
            block = cells[tile(t)].reshape(8, 16, LZ)
            mod_out[f, xs, ys, :] = block
            half_x = block.reshape(4, 2, 16, LZ)
            half_x = half_x[:, 0] + half_x[:, 1]
            for x in range(4):
                fold(start + ((t // 2) * 4 + x) * CY + (t % 2) * 16, half_x[x])
        rows_one = pair_rows(start, 8 * 16)
        one = z_pool(rows_one, slice(0, 128))
        for i in range(PY):
            one_send[f, i] = one[i * 8 : i * 8 + 8]
        routed = across(one_send.at[f], (one_recv_0, one_recv_1)[f], 7 + f)
        pairs = rows_one.reshape(4, 2, 16, LZ)
        fold(start, (pairs[:, 0] + pairs[:, 1]).reshape(4 * 16, LZ))
        rows_two = pair_rows(start, 4 * 8)
        pairs = rows_two.reshape(2, 2, 8, LZ)
        fold(start, (pairs[:, 0] + pairs[:, 1]).reshape(2 * 8, LZ))
        rows_three = pair_rows(start, 2 * 4)
        rest = z_pool(jnp.concatenate([rows_two, rows_three], 0), slice(128, 256))
        for n in range(8):
            i = f * 8 + n
            rest_send[i, pl.ds(0, 4), :] = rest[n * 4 : n * 4 + 4]
            rest_send[i, pl.ds(4, 1), :] = rest[32 + n : 33 + n]
            rest_send[i, pl.ds(5, 3), :] = jnp.zeros((3, L), F32)
            rest_back[i, pl.ds(5, 3), :] = jnp.zeros((3, L), F32)
        return routed

    def choose(source, target, pieces):
        for g in range(PY):
            for level, rows in pieces:
                target[g, rows, :] = source[group_ref[level, g], rows, :]

    landed(back_send.at[0], back_recv.at[0], 8, 3)
    one_0 = coarse(0)
    landed(back_send.at[1], back_recv.at[1], 8, 4)
    one_1 = coarse(1)
    rest_0 = across(rest_send, rest_recv, 9)
    one_0.wait()
    choose(one_recv_0, one_back.at[0], [(0, pl.ds(0, 8))])
    last = [across(one_back.at[0], one_out.at[0], 10)]
    one_1.wait()
    choose(one_recv_1, one_back.at[1], [(0, pl.ds(0, 8))])
    last.append(across(one_back.at[1], one_out.at[1], 11))
    rest_0.wait()
    choose(rest_recv, rest_back, [(1, pl.ds(0, 4)), (2, pl.ds(4, 1))])
    last.append(across(rest_back, rest_out, 12))
    for copy in last:
        copy.wait()


def store_kernel(
    mod_in, one_in, rest_in, mod_out, one_out, two_out, three_out, one_ref, two_ref, three_ref, sems,
):
    outs = [(mod_in, mod_out), (one_ref, one_out), (two_ref, two_out), (three_ref, three_out)]
    stores = [pltpu.make_async_copy(*pair, sems.at[i]) for i, pair in enumerate(outs)]
    stores[0].start()
    for f in range(2):
        one_ref[f] = one_in[f].reshape(8, 16, L)
        for x in range(4):
            for h in range(2):
                two_ref[f, x, pl.ds(h * 4, 4), :] = rest_in[(f * 4 + x) * 2 + h, pl.ds(0, 4), :][:, :64]
        for x in range(2):
            for y in range(4):
                row = rest_in[(f * 2 + x) * 4 + y, pl.ds(4, 1), :]
                three_ref[f, x, pl.ds(y, 1), :] = row[:, 64:96]
    for store in stores[1:]:
        store.start()
    for store in stores:
        store.wait()


def on_device(white_noise, spectrum, group_table):
    shapes = [
        white_noise.shape,
        (2, CX // 2, CY // 2, LZ // 2),
        (2, CX // 4, CY // 4, LZ // 4),
        (2, CX // 8, CY // 8, LZ // 8),
    ]
    hbm = pl.BlockSpec(memory_space=pltpu.HBM)
    wide = pltpu.VMEM((2, DEV * 8, L), F32)
    thin = pltpu.VMEM((DEV * QUAD, L), F32)
    table = pltpu.VMEM((QUAD, L, L), F32)
    one, rest = (2, PY, 8, L), (PY, 8, L)
    slots = 13
    operands = [white_noise, spectrum] + tables()
    results = pl.pallas_call(
        kernel,
        out_shape=[jax.ShapeDtypeStruct(shape, F32) for shape in (shapes[0], one, rest)],
        in_specs=[hbm] * (len(operands) + 1),
        out_specs=[pl.BlockSpec(memory_space=pltpu.VMEM)] * 3,
        scratch_shapes=[pltpu.SMEM(group_table.shape, jnp.int32)]
        + [pltpu.VMEM(value.shape, value.dtype) for value in operands]
        + [thin, thin, pltpu.VMEM((QUAD, L), F32)]
        + [pltpu.VMEM((size, QUAD, L), F32) for size in (PY, DEV)]
        + [table, table, wide, wide, wide, wide, pltpu.VMEM((2, 2, DEV * QUAD, L), F32)]
        + [pltpu.VMEM((2, 2 * 8 * CY, L), F32)]
        + [pltpu.VMEM(shape, F32) for shape in (one, rest, rest, one, rest, rest, rest)]
        + [pltpu.SemaphoreType.DMA]
        + [pltpu.SemaphoreType.DMA((size,)) for size in (len(operands) + 1, slots, slots)],
        compiler_params=pltpu.CompilerParams(
            collective_id=0, has_side_effects=True, vmem_limit_bytes=48 * 1024 * 1024
        ),
    )(*[pltpu.with_memory_space_constraint(v, pltpu.HBM) for v in [group_table] + operands])
    return pl.pallas_call(
        store_kernel,
        out_shape=[jax.ShapeDtypeStruct(shape, F32) for shape in shapes],
        in_specs=[pl.BlockSpec(memory_space=pltpu.VMEM)] * 3,
        out_specs=[hbm] * 4,
        scratch_shapes=[pltpu.VMEM(shape, F32) for shape in shapes[1:]] + [pltpu.SemaphoreType.DMA((4,))],
        compiler_params=pltpu.CompilerParams(vmem_limit_bytes=2 * 1024 * 1024),
    )(*results)


def solution(mesh):
    in_specs = (P(None, "px", "py", None), P("px", "py", None), P())
    out_specs = (P(None, "px", "py", None),) * 4
    return jax.shard_map(
        on_device, mesh=mesh, in_specs=in_specs, out_specs=out_specs, check_vma=False
    )
```

```python
import numpy as np

import jax
import jax.numpy as jnp
from jax import lax
from jax.experimental import pallas as pl
from jax.experimental.pallas import tpu as pltpu
from jax.sharding import PartitionSpec as P

MESH = pl.DeviceIdType.MESH
F32, BF16 = jnp.float32, jnp.bfloat16
PX, PY = 8, 16
DEV = PX * PY
LX, LY, LZ = 128, 512, 256
CX, CY = LX // PX, LY // PY
L = 128
QUAD = 4


def split(values):
    values = np.asarray(values, np.float32)
    high = values.astype(jnp.bfloat16)
    low = (values - high.astype(np.float32)).astype(jnp.bfloat16)
    return np.stack([high, low], 0)


def tables():
    k = np.arange(L)
    z = np.arange(LZ)
    angle = 2.0 * np.pi / LZ * (k[:, None] * z[None, :] % LZ)
    nyquist = np.where(z % 2 == 0, 1.0, -1.0)
    ahead = np.stack([np.cos(angle), -np.sin(angle)], 0)
    back = 2.0 * ahead
    ahead[1, 0] = nyquist
    back[0, 0] = 1.0
    back[1, 0] = nyquist
    z_ahead = split(ahead.reshape(LZ, LZ))
    z_back = split(back.reshape(LZ, LZ) / (LX * LY * LZ))
    first, second = k // 16, k % 16
    turn = first[:, None] * first[None, :] / 8.0 + second[:, None] * second[None, :] / 16.0
    cos, sin = np.cos(2 * np.pi * turn), -np.sin(2 * np.pi * turn)
    column = split(np.block([[cos, -sin], [sin, cos]]))
    row = split(np.block([[cos, sin], [-sin, cos]]))
    twiddle, small = [], []
    for t in range(QUAD):
        xl = (t // 2) * 8 + first
        yl = (t % 2) * 16 + second
        turn = first[:, None] * xl[None, :] / LX + second[:, None] * yl[None, :] / LY
        twiddle.append(np.stack([np.cos(2 * np.pi * turn), -np.sin(2 * np.pi * turn)], 0))
        turn = (t // 2) * first / 16.0 + (t % 2) * second / 32.0
        small.append(np.stack([np.cos(2 * np.pi * turn), -np.sin(2 * np.pi * turn)], 0))
    twiddle = np.concatenate(twiddle, 2).astype(np.float32)
    small = np.stack(small, 1).reshape(2 * QUAD, L).astype(np.float32)
    pool = np.zeros((LZ, LZ))
    pool[z, z // 2] = 1.0 / 8
    pool[z, 128 + z // 4] = 1.0 / 64
    pool[z, 192 + z // 8] = 1.0 / 512
    return [
        jnp.asarray(v)
        for v in (z_ahead, z_back, column, row, twiddle, small, pool.astype(jnp.bfloat16))
    ]


def parts(values):
    high = values.astype(BF16)
    return high, (values - high.astype(F32)).astype(BF16)


def product(left, right, dims):
    return lax.dot_general(left, right, (dims, ((), ())), preferred_element_type=F32)


def left_table(table, values, dims=((1,), (0,))):
    high, low = parts(values)
    first = product(table[0], high, dims) + product(table[0], low, dims)
    return first + product(table[1], high, dims)


def right_table(values, table, dims=((1,), (0,))):
    high, low = parts(values)
    first = product(high, table[0], dims) + product(low, table[0], dims)
    return first + product(high, table[1], dims)


def hops(shift):
    return sum(min(d, 4 - d) for d in shift[:3])


SHIFTS = [(dz, dy, dx, dc) for dz in range(4) for dy in range(4) for dx in range(4) for dc in range(2)]


def spread_evenly(shifts):
    load = np.zeros(6)
    order, left = [], list(shifts)
    while left:
        def cost(shift):
            after = load.copy()
            for axis, d in enumerate(shift[:3]):
                after[2 * axis] += (0, 1, 1, 0)[d]
                after[2 * axis + 1] += (0, 0, 1, 1)[d]
            return after.max() - after.min()
        best = min(left, key=cost)
        for axis, d in enumerate(best[:3]):
            load[2 * axis] += (0, 1, 1, 0)[d]
            load[2 * axis + 1] += (0, 0, 1, 1)[d]
        left.remove(best)
        order.append(best)
    return order


MIXED = spread_evenly([SHIFTS[(i * 37) % 128] for i in range(1, 128)])
SHIFTS = [shift for count in (6, 5, 4, 3, 2, 1, 0) for shift in spread_evenly([m for m in MIXED if hops(m) == count])]

LINE = [(dx, low) for dx in range(4) for low in range(4)]
LINE = sorted(LINE[1:], key=lambda move: -min(move[0], 4 - move[0]) - (move[1] >> 1))


def place():
    px, py = lax.axis_index("px"), lax.axis_index("py")
    return (px >> 2) * 2 + ((py >> 1) & 1), px & 3, py >> 2, py & 1


def shifted(here, dz, dy, dx, dc):
    z, y, x = ((here[i] + d) & 3 for i, d in enumerate((dz, dy, dx)))
    px = (z >> 1) * 4 + y
    py = x * 4 + (z & 1) * 2 + (here[3] ^ dc)
    return px * PY + py, {"px": px, "py": py}


def quarter(t):
    return slice((t // 2) * 8, (t // 2) * 8 + 8), slice((t % 2) * 16, (t % 2) * 16 + 16)


def tile(t):
    return slice(t * L, (t + 1) * L)


def butterfly(values):
    a, b, c, d = values
    p, q, r, s = a + b, a - b, c + d, c - d
    return [p + r, q + s, p - r, q - s]


def turned(real, imag, cos, sin):
    return real * cos - imag * sin, real * sin + imag * cos


def piece(index, height):
    return pl.ds(pl.multiple_of(index * height, height), height)


def kernel(
    group_in, noise_in, spec_in, za_in, zb_in, col_in, row_in, tw_in, small_in, pool_in,
    mod_out, one_out, rest_out,
    group_ref, noise_ref, spec_ref, za_ref, zb_ref, col_ref, row_ref, tw_ref, small_ref, pool_ref,
    s_send, s_recv, n_send, n_line, n_recv, u_table, v_table, ahead_send, ahead_recv, back_send, back_recv, zero_send,
    half_y, one_send, one_recv_0, one_recv_1, one_back, rest_send, rest_recv, rest_back,
    own_sem, fetch_sems, send_sems, recv_sems,
):
    here = place()
    my_px, my_py = lax.axis_index("px"), lax.axis_index("py")
    me = my_px * PY + my_py
    barrier = pltpu.get_barrier_semaphore()

    pairs = (
        (spec_in, spec_ref), (noise_in, noise_ref), (za_in, za_ref), (col_in, col_ref),
        (row_in, row_ref), (tw_in, tw_ref), (small_in, small_ref), (zb_in, zb_ref),
        (pool_in, pool_ref), (group_in, group_ref),
    )
    fetches = [
        pltpu.make_async_copy(source, target, fetch_sems.at[index])
        for index, (source, target) in enumerate(pairs)
    ]
    for fetch in fetches:
        fetch.start()

    for shift in SHIFTS:
        pl.semaphore_signal(barrier, inc=1, device_id=shifted(here, *shift)[1], device_id_type=MESH)

    def spread(send, recv, height, slot, order=MIXED):
        if height == QUAD:
            pltpu.make_async_copy(send.at[piece(me, height)], recv.at[piece(me, height)], own_sem).start()
        else:
            recv[piece(me, height), :] = send[piece(me, height), :]

        def send_to(shift):
            other, device = shifted(here, *shift)
            pltpu.make_async_remote_copy(
                src_ref=send.at[piece(other, height)],
                dst_ref=recv.at[piece(me, height)],
                send_sem=send_sems.at[slot],
                recv_sem=recv_sems.at[slot],
                device_id=device,
                device_id_type=MESH,
            ).start()

        for shift in order:
            send_to(shift)

    def landed(send, recv, height, slot):
        if height == QUAD:
            pltpu.make_async_copy(send.at[piece(me, height)], recv.at[piece(me, height)], own_sem).wait()
        rest = pl.ds(0, (DEV - 1) * height)
        whole = pltpu.make_async_remote_copy(
            src_ref=send.at[rest],
            dst_ref=recv.at[rest],
            send_sem=send_sems.at[slot],
            recv_sem=recv_sems.at[slot],
            device_id=shifted(here, 0, 0, 0, 1)[1],
            device_id_type=MESH,
        )
        whole.wait()

    fetches[0].wait()
    for t in range(QUAD):
        xs, ys = quarter(t)
        block = spec_ref[xs, ys, :].reshape(L, LZ)
        s_send[pl.ds(t, L, stride=QUAD), :] = block[:, :L].T
        n_send[pl.ds(t, 1), :] = block[:, L:].T[:1]

    fetches[1].wait()
    fetches[2].wait()
    za = (za_ref[0], za_ref[1])

    def z_ahead(f):
        rows = [noise_ref[(f,) + quarter(t)].reshape(L, LZ) for t in range(QUAD)]
        return left_table(za, jnp.concatenate(rows, 0), ((1,), (1,)))

    values = [z_ahead(0), z_ahead(1)]
    at_zero = lax.broadcasted_iota(jnp.int32, (L, QUAD * L), 0) == 0
    real_one = jnp.where(at_zero, values[0][L:], values[1][:L])
    imag_zero = jnp.where(at_zero, values[1][:L], values[0][L:])
    members = ((values[0][:L], imag_zero), (real_one, values[1][L:]))
    for f in range(2):
        for c in range(2):
            for t in range(QUAD):
                ahead_send[f, pl.ds(c * QUAD + t, L, stride=8), :] = members[f][c][:, tile(t)]

    pl.semaphore_wait(barrier, DEV - 1)
    line_copy = pltpu.make_async_remote_copy(
        src_ref=n_send,
        dst_ref=n_line.at[my_py],
        send_sem=send_sems.at[5],
        recv_sem=recv_sems.at[5],
        device_id={"py": 0},
        device_id_type=MESH,
    )
    plane_copies = [
        pltpu.make_async_remote_copy(
            src_ref=n_line.at[i],
            dst_ref=n_recv.at[my_px * PY + i],
            send_sem=send_sems.at[6],
            recv_sem=recv_sems.at[6],
            device_id={"px": 0},
            device_id_type=MESH,
        )
        for i in range(PY)
    ]

    def line_rest(device):
        rest = n_line.at[pl.ds(1, PY - 1)]
        return pltpu.make_async_remote_copy(
            src_ref=rest, dst_ref=rest, send_sem=send_sems.at[5], recv_sem=recv_sems.at[5],
            device_id=device, device_id_type=MESH,
        )

    def plane_rest(rest, device):
        return pltpu.make_async_remote_copy(
            src_ref=rest, dst_ref=rest, send_sem=send_sems.at[6], recv_sem=recv_sems.at[6],
            device_id=device, device_id_type=MESH,
        )

    pl.when(my_py != 0)(line_copy.start)
    spread(s_send, s_recv, QUAD, 0)

    spread(ahead_send.at[0], ahead_recv.at[0], 8, 1)

    @pl.when(my_py == 0)
    def _():
        n_line[0] = n_send[...]
        line_rest({"py": 1}).wait_recv()

        @pl.when(my_px != 0)
        def _():
            for copy in plane_copies:
                copy.start()

    spread(ahead_send.at[1], ahead_recv.at[1], 8, 2, SHIFTS)

    landed(s_send, s_recv, QUAD, 0)
    for t in range(QUAD):
        u_table[t] = s_recv[pl.ds(t, L, stride=QUAD), :].T

    pl.when(my_py != 0)(line_copy.wait_send)
    for index in range(3, 7):
        fetches[index].wait()

    def last_table():
        @pl.when(me != 0)
        def _():
            v_table[...] = u_table[...]

        @pl.when((my_py == 0) & (my_px != 0))
        def _():
            plane_rest(n_line, {"px": 0}).wait_send()

        @pl.when(me == 0)
        def _():
            n_recv[pl.ds(0, PY)] = n_line[...]
            plane_rest(n_recv.at[pl.ds(PY, DEV - PY)], {"px": 1}).wait_recv()
            for t in range(QUAD):
                v_table[t] = n_recv[:, t, :].T

    column = (col_ref[0], col_ref[1])
    row = (row_ref[0], row_ref[1])
    for f in range(2):
        landed(ahead_send.at[f], ahead_recv.at[f], 8, 1 + f)
        if f == 1:
            last_table()
        plane = [
            jnp.concatenate(
                [ahead_recv[f, pl.ds(c * QUAD + t, L, stride=8), :] for t in range(QUAD)], 1
            )
            for c in range(2)
        ]
        mixed = left_table(column, jnp.concatenate(plane, 0))
        real, imag = turned(mixed[:L], mixed[L:], tw_ref[0], tw_ref[1])
        reals = butterfly([real[:, tile(t)] for t in range(QUAD)])
        imags = butterfly([imag[:, tile(t)] for t in range(QUAD)])
        rows = []
        for t in range(QUAD):
            cos, sin = small_ref[pl.ds(t, 1), :], small_ref[pl.ds(QUAD + t, 1), :]
            pair = turned(reals[t], imags[t], cos, sin) if t else (reals[t], imags[t])
            rows.append(jnp.concatenate(pair, 1))
        freq = right_table(jnp.concatenate(rows, 0), row)
        table = u_table if f == 0 else v_table
        scale = jnp.concatenate([table[t] for t in range(QUAD)], 0)
        freq = freq * jnp.concatenate([scale, scale], 1)
        mixed = right_table(freq, column)
        reals, imags = [], []
        for t in range(QUAD):
            part = mixed[tile(t)]
            pair = (part[:, :L], part[:, L:])
            if t:
                cos, sin = small_ref[pl.ds(t, 1), :], small_ref[pl.ds(QUAD + t, 1), :]
                pair = turned(*pair, cos, -sin)
            reals.append(pair[0])
            imags.append(pair[1])
        real = jnp.concatenate(butterfly(reals), 1)
        imag = jnp.concatenate(butterfly(imags), 1)
        real, imag = turned(real, imag, tw_ref[0], -tw_ref[1])
        plane = left_table(row, jnp.concatenate([real, imag], 0))
        @pl.when(me != 0)
        def _():
            for c in range(2):
                for t in range(QUAD):
                    back_send[f, pl.ds(c * QUAD + t, L, stride=8), :] = plane[tile(c), tile(t)]
            spread(back_send.at[f], back_recv.at[f], 8, 3 + f, SHIFTS)

        @pl.when(me == 0)
        def _():
            for c in range(2):
                for t in range(QUAD):
                    zero_send[f, c, pl.ds(t, L, stride=QUAD), :] = plane[tile(c), tile(t)]
                back_recv[c, pl.ds(f * QUAD, QUAD), :] = zero_send[f, c, pl.ds(0, QUAD), :]

            def send_to(shift):
                other, device = shifted(here, *shift)
                for c in range(2):
                    pltpu.make_async_remote_copy(
                        src_ref=zero_send.at[f, c, piece(other, QUAD)],
                        dst_ref=back_recv.at[c, pl.ds(f * QUAD, QUAD)],
                        send_sem=send_sems.at[3 + c],
                        recv_sem=recv_sems.at[3 + c],
                        device_id=device,
                        device_id_type=MESH,
                    ).start()

            @pl.loop(0, 16)
            def _(step):
                dx, dy = step & 3, step >> 2
                pl.when(step != 0)(lambda: send_to((0, dy, dx, 0)))
                for n in range(1, 8):
                    dz, dc = n >> 1, n & 1
                    send_to((dz, dy + n, dx + dz, dc))

    for index in range(7, 10):
        fetches[index].wait()
    zb = (zb_ref[0], zb_ref[1])

    def fold(start, rows):
        for h in range(2):
            half_y[h, pl.ds(start, rows.shape[0]), :] = rows[:, tile(h)]

    def pair_rows(start, count):
        rows = [
            half_y[h, pl.ds(start, count, stride=2), :] + half_y[h, pl.ds(start + 1, count, stride=2), :]
            for h in range(2)
        ]
        return jnp.concatenate(rows, 1)

    def z_pool(values, lanes):
        high, low = parts(values)
        pool = pool_ref[:, lanes]
        return product(high, pool, ((1,), (0,))) + product(low, pool, ((1,), (0,)))

    def across(send, recv, slot):
        recv[my_py] = send[my_py]
        for dx, low in LINE:
            other = (((my_py >> 2) + dx) & 3) * 4 + ((my_py & 3) ^ low)
            pltpu.make_async_remote_copy(
                src_ref=send.at[other],
                dst_ref=recv.at[my_py],
                send_sem=send_sems.at[slot],
                recv_sem=recv_sems.at[slot],
                device_id={"py": other},
                device_id_type=MESH,
            ).start()
        rest = pl.ds(0, PY - 1)
        whole = pltpu.make_async_remote_copy(
            src_ref=send.at[rest],
            dst_ref=recv.at[rest],
            send_sem=send_sems.at[slot],
            recv_sem=recv_sems.at[slot],
            device_id={"py": my_py ^ 1},
            device_id_type=MESH,
        )
        return whole

    def coarse(f):
        tiles = [
            [back_recv[f, pl.ds(c * QUAD + t, L, stride=8), :] for t in range(QUAD)]
            for c in range(2)
        ]
        waves = jnp.concatenate([jnp.concatenate(part, 1) for part in tiles], 0)
        cells = right_table(waves, zb, ((0,), (0,)))
        cells = jnp.exp(0.5 * cells)
        start = f * 4 * CY * 2
        for t in range(QUAD):
            xs, ys = quarter(t)
            block = cells[tile(t)].reshape(8, 16, LZ)
            mod_out[f, xs, ys, :] = block
            half_x = block.reshape(4, 2, 16, LZ)
            half_x = half_x[:, 0] + half_x[:, 1]
            for x in range(4):
                fold(start + ((t // 2) * 4 + x) * CY + (t % 2) * 16, half_x[x])
        rows_one = pair_rows(start, 8 * 16)
        one = z_pool(rows_one, slice(0, 128))
        for i in range(PY):
            one_send[f, i] = one[i * 8 : i * 8 + 8]
        routed = across(one_send.at[f], (one_recv_0, one_recv_1)[f], 7 + f)
        pairs = rows_one.reshape(4, 2, 16, LZ)
        fold(start, (pairs[:, 0] + pairs[:, 1]).reshape(4 * 16, LZ))
        rows_two = pair_rows(start, 4 * 8)
        pairs = rows_two.reshape(2, 2, 8, LZ)
        fold(start, (pairs[:, 0] + pairs[:, 1]).reshape(2 * 8, LZ))
        rows_three = pair_rows(start, 2 * 4)
        rest = z_pool(jnp.concatenate([rows_two, rows_three], 0), slice(128, 256))
        for n in range(8):
            i = f * 8 + n
            rest_send[i, pl.ds(0, 4), :] = rest[n * 4 : n * 4 + 4]
            rest_send[i, pl.ds(4, 1), :] = rest[32 + n : 33 + n]
            rest_send[i, pl.ds(5, 3), :] = jnp.zeros((3, L), F32)
            rest_back[i, pl.ds(5, 3), :] = jnp.zeros((3, L), F32)
        return routed

    def choose(source, target, pieces):
        for g in range(PY):
            for level, rows in pieces:
                target[g, rows, :] = source[group_ref[level, g], rows, :]

    landed(back_send.at[0], back_recv.at[0], 8, 3)
    one_0 = coarse(0)
    landed(back_send.at[1], back_recv.at[1], 8, 4)
    one_1 = coarse(1)
    rest_0 = across(rest_send, rest_recv, 9)
    one_0.wait()
    choose(one_recv_0, one_back.at[0], [(0, pl.ds(0, 8))])
    last = [across(one_back.at[0], one_out.at[0], 10)]
    one_1.wait()
    choose(one_recv_1, one_back.at[1], [(0, pl.ds(0, 8))])
    last.append(across(one_back.at[1], one_out.at[1], 11))
    rest_0.wait()
    choose(rest_recv, rest_back, [(1, pl.ds(0, 4)), (2, pl.ds(4, 1))])
    last.append(across(rest_back, rest_out, 12))
    for copy in last:
        copy.wait()


def store_kernel(
    mod_in, one_in, rest_in, mod_out, one_out, two_out, three_out, one_ref, two_ref, three_ref, sems,
):
    outs = [(mod_in, mod_out), (one_ref, one_out), (two_ref, two_out), (three_ref, three_out)]
    stores = [pltpu.make_async_copy(*pair, sems.at[i]) for i, pair in enumerate(outs)]
    stores[0].start()
    for f in range(2):
        one_ref[f] = one_in[f].reshape(8, 16, L)
        for x in range(4):
            for h in range(2):
                two_ref[f, x, pl.ds(h * 4, 4), :] = rest_in[(f * 4 + x) * 2 + h, pl.ds(0, 4), :][:, :64]
        for x in range(2):
            for y in range(4):
                row = rest_in[(f * 2 + x) * 4 + y, pl.ds(4, 1), :]
                three_ref[f, x, pl.ds(y, 1), :] = row[:, 64:96]
    for store in stores[1:]:
        store.start()
    for store in stores:
        store.wait()


def on_device(white_noise, spectrum, group_table):
    shapes = [
        white_noise.shape,
        (2, CX // 2, CY // 2, LZ // 2),
        (2, CX // 4, CY // 4, LZ // 4),
        (2, CX // 8, CY // 8, LZ // 8),
    ]
    hbm = pl.BlockSpec(memory_space=pltpu.HBM)
    wide = pltpu.VMEM((2, DEV * 8, L), F32)
    thin = pltpu.VMEM((DEV * QUAD, L), F32)
    table = pltpu.VMEM((QUAD, L, L), F32)
    one, rest = (2, PY, 8, L), (PY, 8, L)
    slots = 13
    operands = [white_noise, spectrum] + tables()
    results = pl.pallas_call(
        kernel,
        out_shape=[jax.ShapeDtypeStruct(shape, F32) for shape in (shapes[0], one, rest)],
        in_specs=[hbm] * (len(operands) + 1),
        out_specs=[pl.BlockSpec(memory_space=pltpu.VMEM)] * 3,
        scratch_shapes=[pltpu.SMEM(group_table.shape, jnp.int32)]
        + [pltpu.VMEM(value.shape, value.dtype) for value in operands]
        + [thin, thin, pltpu.VMEM((QUAD, L), F32)]
        + [pltpu.VMEM((size, QUAD, L), F32) for size in (PY, DEV)]
        + [table, table, wide, wide, wide, wide, pltpu.VMEM((2, 2, DEV * QUAD, L), F32)]
        + [pltpu.VMEM((2, 2 * 8 * CY, L), F32)]
        + [pltpu.VMEM(shape, F32) for shape in (one, rest, rest, one, rest, rest, rest)]
        + [pltpu.SemaphoreType.DMA]
        + [pltpu.SemaphoreType.DMA((size,)) for size in (len(operands) + 1, slots, slots)],
        compiler_params=pltpu.CompilerParams(
            collective_id=0, has_side_effects=True, vmem_limit_bytes=48 * 1024 * 1024
        ),
    )(*[pltpu.with_memory_space_constraint(v, pltpu.HBM) for v in [group_table] + operands])
    return pl.pallas_call(
        store_kernel,
        out_shape=[jax.ShapeDtypeStruct(shape, F32) for shape in shapes],
        in_specs=[pl.BlockSpec(memory_space=pltpu.VMEM)] * 3,
        out_specs=[hbm] * 4,
        scratch_shapes=[pltpu.VMEM(shape, F32) for shape in shapes[1:]] + [pltpu.SemaphoreType.DMA((4,))],
        compiler_params=pltpu.CompilerParams(vmem_limit_bytes=2 * 1024 * 1024),
    )(*results)


def solution(mesh):
    in_specs = (P(None, "px", "py", None), P("px", "py", None), P())
    out_specs = (P(None, "px", "py", None),) * 4
    return jax.shard_map(
        on_device, mesh=mesh, in_specs=in_specs, out_specs=out_specs, check_vma=False
    )
```
